16 devices in a mesh: dp: 4 (over y, z, core), tp: 4 (over x).
Axes of the slice: x: 4, y: 2, z: 1, core: 2. Of those that a mesh axis runs over, the one named last changes fastest.
The devices are a block of a 4x4x8 slice.
Arguments:
- x: bfloat16 [8192, 6144], P('dp'), parts along dimension 0
- w_gate: bfloat16 [6144, 16384], P(None, 'tp')
- w_up: bfloat16 [6144, 16384], P(None, 'tp')
- w_down: bfloat16 [16384, 6144], P('tp')
Outputs:
- output: bfloat16 [8192, 6144], P('dp'), parts along dimension 0
There are 4 independent parts. The reference program is written for one: setup_inputs(seed, part) draws one part's arguments, and reference() takes and returns one part's arrays. A program takes and returns all parts, laid end to end along the dimension named above; an argument that names none is the same for every part.
All inputs are finite; a program needn't handle non-finite values.
Results may differ from the reference program's by a relative error of at most 0.016.
Values are sent between devices in bfloat16 or wider.
A program may use at most 768 MiB of HBM per device.

```python
import jax
import jax.numpy as jnp

ROWS = 2048
D = 6144
FF = 16384


def setup_inputs(seed: int = 0, part: int = 0) -> dict:
    kx, kg, ku, kd = jax.random.split(jax.random.key(seed), 4)
    drawn = {
        "x": jax.random.normal(jax.random.fold_in(kx, part), (ROWS, D), jnp.float32),
        "w_gate": jax.random.normal(kg, (D, FF), jnp.float32) * D**-0.5,
        "w_up": jax.random.normal(ku, (D, FF), jnp.float32) * D**-0.5,
        "w_down": jax.random.normal(kd, (FF, D), jnp.float32) * FF**-0.5,
    }
    return {k: v.astype(jnp.bfloat16) for k, v in drawn.items()}


def reference(x, w_gate, w_up, w_down):
    gate = jnp.dot(x, w_gate, preferred_element_type=jnp.float32)
    up = jnp.dot(x, w_up, preferred_element_type=jnp.float32)
    hidden = (jax.nn.silu(gate) * up).astype(jnp.bfloat16)
    return jnp.dot(hidden, w_down, preferred_element_type=jnp.float32).astype(jnp.bfloat16)
```

```python
import functools

import jax
import jax.numpy as jnp
from jax import lax
from jax.experimental import pallas as pl
from jax.experimental.pallas import tpu as pltpu
from jax.sharding import PartitionSpec as P

MESH = pl.DeviceIdType.MESH
F32, BF16 = jnp.float32, jnp.bfloat16

BLOCKS = (256, 256, 320, 320, 320, 320, 256)
UNIT = 64
DEPTH = 10
WBUF = 3
TN = 256
TD = 512

SCHEDULE = {
    "pair": [24, 25, 26, 27, 52, 53, 54, 55, 80, 81, 82, 83, 84, 110, 111, 112, 113, 114, 139, 140, 141, 142, 143, 169, 170, 171, 172, 173, 196, 197, 198, 199],
    "own": [31, 33, 34, 35, 59, 60, 61, 62, 87, 90, 91, 92, 93, 117, 118, 119, 120, 121, 145, 148, 149, 150, 151, 176, 177, 178, 179, 180, 200, 201, 202, 203],
    "relay": [37, 39, 41, 43, 64, 65, 67, 69, 93, 95, 96, 98, 100, 122, 123, 125, 127, 129, 151, 152, 154, 156, 158, 182, 184, 186, 189, 192, 204, 205, 206, 207],
    "free": [39, 41, 43, 64, 65, 67, 69, 93, 95, 96, 98, 100, 122, 123, 125, 127, 129, 151, 152, 154, 156, 158, 182, 184, 186, 189, 192, 204, 205, 206, 207, 208],
}
EVENTS = tuple(SCHEDULE)


def pick(index, values):
    total = jnp.int32(0)
    for i, v in enumerate(values):
        if v:
            total = total + jnp.where(index == i, jnp.int32(v), jnp.int32(0))
    return total


def kernel(n, x_ref, wg_ref, wu_ref, wd_ref, y_ref, xv, wv, hv, hold,
           opp_s, dir_s, sum_s, own_s, opp_r, dir_r, sum_r,
           x_sem, w_sem, loc_sem, opp_ss, opp_rs, dir_ss, dir_rs, sum_ss, sum_rs,
           ag_ss, ag_rs, re_ss, re_rs):
    me = lax.axis_index("tp")
    rows, depth_in = x_ref.shape
    hidden, width = wd_ref.shape
    piece = width // n
    nu = rows // UNIT
    gu_steps, dn_steps = hidden // TN, width // TD
    per_piece = dn_steps // n
    steps = gu_steps + dn_steps
    nb = len(BLOCKS)
    total_steps = nb * steps
    last = max(max(v) for v in SCHEDULE.values())
    windows = max(nb, last // steps + 1)
    masks = {e: [sum(1 << (g % steps) for g in v if g // steps == b) for b in range(windows)] for e, v in SCHEDULE.items()}
    starts = {e: [sum(g // steps < b for g in v) for b in range(windows)] for e, v in SCHEDULE.items()}
    row0 = [sum(BLOCKS[:b]) for b in range(nb)]

    def at(offset):
        return lax.rem(me + offset, n)

    def remote(src, dst, ssem, rsem, target):
        return pltpu.make_async_remote_copy(src_ref=src, dst_ref=dst, send_sem=ssem, recv_sem=rsem,
                                            device_id={"tp": target}, device_id_type=MESH)

    def cols(owner):
        return pl.ds(pl.multiple_of(owner * piece, piece), piece)

    def unit_rows(s):
        return pl.ds(pl.multiple_of(s * UNIT, UNIT), UNIT)

    def gu_copies(t, slot):
        c = pl.ds(pl.multiple_of(t * TN, TN), TN)
        return (pltpu.make_async_copy(wg_ref.at[:, c], wv.at[slot, :, 0:TN], w_sem.at[slot, 0]),
                pltpu.make_async_copy(wu_ref.at[:, c], wv.at[slot, :, TN:2 * TN], w_sem.at[slot, 1]))

    def dn_copy(t, slot):
        p, j = t // per_piece, lax.rem(t, per_piece)
        c = pl.ds(pl.multiple_of(at(pick(p, (2, 1, 3, 0))) * piece + j * TD, TD), TD)
        return pltpu.make_async_copy(wd_ref.at[:, c], wv.at[slot, 0:hidden, :], w_sem.at[slot, 0])

    def start_gu(t, slot):
        for c in gu_copies(t, slot):
            c.start()

    def x_copy(b, r):
        return pltpu.make_async_copy(x_ref.at[pl.ds(pl.multiple_of(pick(b, row0), UNIT), r), :], xv.at[pl.ds(0, r), :], x_sem)

    def opp_copy(s, slot, par, c):
        return remote(opp_s.at[slot, :, c], opp_r.at[slot, :, c], opp_ss.at[slot], opp_rs.at[slot], at(1 + 2 * par))

    def dir_copy(s, slot, par):
        return remote(dir_s.at[slot], dir_r.at[slot], dir_ss.at[slot], dir_rs.at[slot], at(3 - 2 * par))

    def sum_copy(s, slot, par):
        return remote(sum_s.at[slot], sum_r.at[slot], sum_ss.at[slot], sum_rs.at[slot], at(1 + 2 * par))

    def own_copy(s, slot, side):
        return remote(own_s.at[slot], y_ref.at[unit_rows(s), cols(me)], ag_ss.at[slot, side], ag_rs.at[s, side], at(1 + 2 * side))

    def relay_copy(s, par):
        view = y_ref.at[unit_rows(s), cols(at(3 - 2 * par))]
        return remote(view, view, re_ss.at[s], re_rs.at[s], at(1 + 2 * par))

    def loc_copy(s, slot):
        return pltpu.make_async_copy(own_s.at[slot], y_ref.at[unit_rows(s), cols(me)], loc_sem.at[slot])

    whole = pl.ds(0, piece)

    def pair(s):
        slot, par = lax.rem(s, DEPTH), lax.rem(s, 2)
        opp_copy(s, slot, par, whole).wait_recv()
        sum_s[slot] = (hold[slot, 1 + par] + opp_r[slot].astype(F32)).astype(BF16)
        sum_copy(s, slot, par).start()

    def own(s):
        slot, par = lax.rem(s, DEPTH), lax.rem(s, 2)
        dir_copy(s, slot, par).wait_recv()
        sum_copy(s, slot, par).wait_recv()
        own_s[slot] = (hold[slot, 3] + sum_r[slot].astype(F32) + dir_r[slot].astype(F32)).astype(BF16)
        own_copy(s, slot, 0).start()
        own_copy(s, slot, 1).start()
        loc_copy(s, slot).start()

    def relay(s):
        slot, par = lax.rem(s, DEPTH), lax.rem(s, 2)
        own_copy(s, slot, 0).wait_recv()
        own_copy(s, slot, 1).wait_recv()
        relay_copy(s, par).start()

    def free(s):
        slot, par = lax.rem(s, DEPTH), lax.rem(s, 2)
        opp_copy(s, slot, par, whole).wait_send()
        dir_copy(s, slot, par).wait_send()
        sum_copy(s, slot, par).wait_send()
        own_copy(s, slot, 0).wait_send()
        own_copy(s, slot, 1).wait_send()
        loc_copy(s, slot).wait()

    actions = {"pair": pair, "own": own, "relay": relay, "free": free}

    def events(t, mask, done):
        out = []
        for e in EVENTS:
            hit = lax.shift_right_logical(mask[e], t) & 1

            @pl.when(hit == 1)
            def _(e=e, c=done[len(out)]):
                actions[e](c)

            out.append(done[len(out)] + hit)
        return tuple(out)

    x_copy(jnp.int32(0), BLOCKS[0]).start()
    for t in range(WBUF - 1):
        start_gu(jnp.int32(t), jnp.int32(t))
    barrier = pltpu.get_barrier_semaphore()
    for offset in (1, n - 1):
        pl.semaphore_signal(barrier, inc=1, device_id={"tp": at(offset)}, device_id_type=MESH)
    pl.semaphore_wait(barrier, 2)

    def block(b, r):
        units = r // UNIT
        first = pick(b, [v // UNIT for v in row0])
        base = b * steps
        mask = {e: pick(b, masks[e]) for e in EVENTS}
        done = tuple(pick(b, starts[e]) for e in EVENTS)
        x_copy(b, r).wait()

        def gu_step(t, done):
            slot = lax.rem(base + t, WBUF)
            for c in gu_copies(t, slot):
                c.wait()
            ahead = t + WBUF - 1
            later = lax.rem(base + ahead, WBUF)

            @pl.when(ahead < gu_steps)
            def _():
                start_gu(ahead, later)

            @pl.when(ahead >= gu_steps)
            def _():
                dn_copy(ahead - gu_steps, later).start()

            xb = xv[0:r, :]
            gate = jnp.dot(xb, wv[slot, :, 0:TN], preferred_element_type=F32)
            up = jnp.dot(xb, wv[slot, :, TN:2 * TN], preferred_element_type=F32)
            hv[0:r, pl.ds(pl.multiple_of(t * TN, TN), TN)] = (jax.nn.silu(gate) * up).astype(BF16)
            return events(t, mask, done)

        done = lax.fori_loop(0, gu_steps, gu_step, done)
        for r2 in sorted(set(BLOCKS)):
            @pl.when(pick(b + 1, [v == r2 for v in BLOCKS]) == 1)
            def _(r2=r2):
                x_copy(b + 1, r2).start()

        def dn_step(t, done):
            g = base + gu_steps + t
            slot = lax.rem(g, WBUF)
            dn_copy(t, slot).wait()
            ahead = t + WBUF - 1
            later = lax.rem(g + WBUF - 1, WBUF)

            @pl.when(ahead < dn_steps)
            def _():
                dn_copy(ahead, later).start()

            @pl.when((ahead >= dn_steps) & (b + 1 < nb))
            def _():
                start_gu(ahead - dn_steps, later)

            p, j = t // per_piece, lax.rem(t, per_piece)
            c = pl.ds(pl.multiple_of(j * TD, TD), TD)
            term = jnp.dot(hv[0:r, :], wv[slot, 0:hidden, :], preferred_element_type=F32)
            for k in range(units):
                hold[lax.rem(first + k, DEPTH), p, :, c] = term[k * UNIT:(k + 1) * UNIT, :]

            @pl.when(p == 0)
            def _():
                def send(k, _):
                    s = first + k
                    slot, par = lax.rem(s, DEPTH), lax.rem(s, 2)
                    opp_s[slot, :, c] = hold[slot, 0, :, c].astype(BF16)
                    opp_copy(s, slot, par, c).start()
                    return 0
                lax.fori_loop(0, units, send, 0)

            @pl.when((j == per_piece - 1) & ((p == 1) | (p == 2)))
            def _():
                def send(k, _):
                    s = first + k
                    slot, par = lax.rem(s, DEPTH), lax.rem(s, 2)

                    @pl.when(p == 2 - par)
                    def _():
                        dir_s[slot] = hold[slot, 2 - par].astype(BF16)
                        dir_copy(s, slot, par).start()
                    return 0
                lax.fori_loop(0, units, send, 0)

            return events(gu_steps + t, mask, done)

        lax.fori_loop(0, dn_steps, dn_step, done)

    def outer(b, _):
        for r in sorted(set(BLOCKS)):
            @pl.when(pick(b, [v == r for v in BLOCKS]) == 1)
            def _(r=r):
                block(b, r)
        return 0

    lax.fori_loop(0, nb, outer, 0)

    def tail(g, done):
        b = g // steps
        return events(lax.rem(g, steps), {e: pick(b, masks[e]) for e in EVENTS}, done)

    lax.fori_loop(total_steps, last + 1, tail, tuple(jnp.int32(sum(g < total_steps for g in v)) for v in SCHEDULE.values()))

    def drain(s, _):
        par = lax.rem(s, 2)
        relay_copy(s, par).wait()
        return 0

    lax.fori_loop(0, nu, drain, 0)


def solution(mesh):
    n = mesh.shape["tp"]

    def step(x, w_gate, w_up, w_down):
        rows, din = x.shape
        hidden, width = w_down.shape
        piece = width // n
        rmax = max(BLOCKS)
        ring = pltpu.VMEM((DEPTH, UNIT, piece), BF16)
        dma = pltpu.SemaphoreType.DMA
        return pl.pallas_call(
            functools.partial(kernel, n),
            out_shape=jax.ShapeDtypeStruct((rows, width), BF16),
            in_specs=[pl.BlockSpec(memory_space=pl.ANY)] * 4,
            out_specs=pl.BlockSpec(memory_space=pl.ANY),
            scratch_shapes=[
                pltpu.VMEM((rmax, din), BF16),
                pltpu.VMEM((WBUF, din, 2 * TN), BF16),
                pltpu.VMEM((rmax, hidden), BF16),
                pltpu.VMEM((DEPTH, n, UNIT, piece), F32),
                ring, ring, ring, ring, ring, ring, ring,
                dma, dma((WBUF, 2)), dma((DEPTH,)),
                dma((DEPTH,)), dma((DEPTH,)), dma((DEPTH,)), dma((DEPTH,)), dma((DEPTH,)), dma((DEPTH,)),
                dma((DEPTH, 2)), dma((rows // UNIT, 2)), dma((rows // UNIT,)), dma((rows // UNIT,)),
            ],
            compiler_params=pltpu.CompilerParams(
                collective_id=0, has_side_effects=True, vmem_limit_bytes=63 * 2**20),
            cost_estimate=pl.CostEstimate(flops=6 * rows * din * hidden, bytes_accessed=7 * 6 * din * hidden, transcendentals=0),
        )(x, w_gate, w_up, w_down)

    return jax.shard_map(
        step,
        mesh=mesh,
        in_specs=(P("dp", None), P(None, "tp"), P(None, "tp"), P("tp", None)),
        out_specs=P("dp", None),
        check_vma=False,
    )
```

```python
import functools

import jax
import jax.numpy as jnp
from jax import lax
from jax.experimental import pallas as pl
from jax.experimental.pallas import tpu as pltpu
from jax.sharding import PartitionSpec as P

MESH = pl.DeviceIdType.MESH
F32, BF16 = jnp.float32, jnp.bfloat16

BLOCKS = (256, 256, 320, 320, 320, 320, 256)
UNIT = 64
DEPTH = 10
WBUF = 3
TN = 256
TD = 768
TAIL = 8
CHUNK = 128

SCHEDULE = {
    "pair": [21, 22, 23, 24, 47, 48, 49, 50, 69, 70, 71, 72, 73, 94, 96, 97, 98, 99, 119, 120, 121, 122, 123, 145, 146, 147, 148, 149, 169, 170, 171, 172],
    "own": [28, 29, 31, 32, 53, 54, 55, 56, 76, 77, 78, 79, 80, 101, 104, 105, 106, 107, 128, 129, 130, 131, 132, 156, 160, 161, 162, 163, 176, 177, 178, 179],
    "relay": [33, 35, 37, 40, 57, 59, 60, 62, 81, 83, 85, 86, 88, 107, 109, 111, 113, 114, 134, 135, 137, 139, 140, 163, 168, 173, 174, 175, 180, 181, 182, 183],
    "free": [35, 37, 40, 57, 59, 60, 62, 81, 83, 85, 86, 88, 107, 109, 111, 113, 114, 134, 135, 137, 139, 140, 163, 168, 173, 174, 175, 180, 181, 182, 183, 184],
}
EVENTS = tuple(SCHEDULE)


def pick(index, values):
    total = jnp.int32(0)
    for i, v in enumerate(values):
        if v:
            total = total + jnp.where(index == i, jnp.int32(v), jnp.int32(0))
    return total


def kernel(n, x_ref, wg_ref, wu_ref, wd_ref, y_ref, rel_r_ref, rel_l_ref, xv, wv, hv, hold,
           opp_s, dir_s, sum_s, own_s, opp_r, dir_r, sum_r,
           x_sem, w_sem, out_sem, opp_rs, own_rs, ag_rs, re_ss, re_rs):
    me = lax.axis_index("tp")
    rows, depth_in = x_ref.shape
    hidden, width = wd_ref.shape
    piece = width // n
    nu = rows // UNIT
    kept = nu - TAIL
    gu_steps, dn_steps = hidden // TN, width // TD
    per_piece = dn_steps // n
    steps = gu_steps + dn_steps
    nb = len(BLOCKS)
    total_steps = nb * steps
    last = max(max(v) for v in SCHEDULE.values())
    windows = max(nb, last // steps + 1)
    masks = {e: [sum(1 << (g % steps) for g in v if g // steps == b) for b in range(windows)] for e, v in SCHEDULE.items()}
    starts = {e: [sum(g // steps < b for g in v) for b in range(windows)] for e, v in SCHEDULE.items()}
    mid = {e: [sum(g // steps < b or (g // steps == b and g % steps < gu_steps) for g in v) for b in range(windows)] for e, v in SCHEDULE.items()}
    row0 = [sum(BLOCKS[:b]) for b in range(nb)]

    def at(offset):
        return lax.rem(me + offset, n)

    def remote(src, dst, ssem, rsem, target):
        return pltpu.make_async_remote_copy(src_ref=src, dst_ref=dst, send_sem=ssem, recv_sem=rsem,
                                            device_id={"tp": target}, device_id_type=MESH)

    def cols(owner):
        return pl.ds(pl.multiple_of(owner * piece, piece), piece)

    def unit_rows(s):
        return pl.ds(pl.multiple_of(s * UNIT, UNIT), UNIT)

    def gu_copies(t, slot):
        c = pl.ds(pl.multiple_of(t * TN, TN), TN)
        return (pltpu.make_async_copy(wg_ref.at[:, c], wv.at[slot, :, 0:TN], w_sem.at[slot]),
                pltpu.make_async_copy(wu_ref.at[:, c], wv.at[slot, :, TN:2 * TN], w_sem.at[slot]))

    side, half = TD - 2 * TN, hidden // 2

    def dn_copies(t, slot):
        p, j = t // per_piece, lax.rem(t, per_piece)
        c = at(pick(p, (2, 1, 3, 0))) * piece + j * TD
        main = pl.ds(pl.multiple_of(c, TN), 2 * TN)
        rest = pl.ds(pl.multiple_of(c + 2 * TN, TN), side)
        return (pltpu.make_async_copy(wd_ref.at[:, main], wv.at[slot, 0:hidden, :], w_sem.at[slot]),
                pltpu.make_async_copy(wd_ref.at[0:half, rest], wv.at[slot, hidden:hidden + half, 0:side], w_sem.at[slot]),
                pltpu.make_async_copy(wd_ref.at[half:hidden, rest], wv.at[slot, hidden:hidden + half, side:2 * side], w_sem.at[slot]))

    def start_dn(t, slot):
        for c in dn_copies(t, slot):
            c.start()

    def tile_wait(slot):
        pltpu.make_async_copy(wv.at[slot], wv.at[slot], w_sem.at[slot]).wait()

    def start_gu(t, slot):
        for c in gu_copies(t, slot):
            c.start()

    def x_copy(b, r):
        return pltpu.make_async_copy(x_ref.at[pl.ds(pl.multiple_of(pick(b, row0), UNIT), r), :], xv.at[pl.ds(0, r), :], x_sem)

    def opp_copy(s, slot, par, c):
        return remote(opp_s.at[slot, :, c], opp_r.at[slot, :, c], out_sem.at[slot], opp_rs.at[slot], at(1 + 2 * par))

    def dir_copy(s, slot, par, c):
        return remote(dir_s.at[slot, :, c], dir_r.at[slot, :, c], out_sem.at[slot], own_rs.at[slot], at(3 - 2 * par))

    def sum_copy(s, slot, par):
        return remote(sum_s.at[slot], sum_r.at[slot], out_sem.at[slot], own_rs.at[slot], at(1 + 2 * par))

    def own_copy(s, slot, side):
        return remote(own_s.at[slot], y_ref.at[unit_rows(s), cols(me)], out_sem.at[slot], ag_rs.at[slot], at(1 + 2 * side))

    def keep_copy(s, slot, side):
        rel = (rel_r_ref, rel_l_ref)[side].at[(s - kept) // 2]
        return remote(own_s.at[slot], rel, out_sem.at[slot], ag_rs.at[slot], at(1 + 2 * side))

    def relay_copy(s, par):
        view = y_ref.at[unit_rows(s), cols(at(3 - 2 * par))]
        k = lax.rem(s, DEPTH + TAIL)
        return remote(view, view, re_ss.at[k], re_rs.at[k], at(1 + 2 * par))

    def loc_copy(s, slot):
        return pltpu.make_async_copy(own_s.at[slot], y_ref.at[unit_rows(s), cols(me)], out_sem.at[slot])

    whole = pl.ds(0, piece)

    def arrived(sem, pieces):
        size = hold.at[0, 0:pieces // 2]
        pltpu.make_async_copy(size, size, sem).wait()

    def pair(s):
        slot, par = lax.rem(s, DEPTH), lax.rem(s, 2)
        opp_copy(s, slot, par, whole).wait_recv()
        sum_s[slot] = (hold[slot, 1 + par] + opp_r[slot].astype(F32)).astype(BF16)
        sum_copy(s, slot, par).start()

    def own(s):
        slot, par = lax.rem(s, DEPTH), lax.rem(s, 2)
        arrived(own_rs.at[slot], 2)
        own_s[slot] = (hold[slot, 3] + sum_r[slot].astype(F32) + dir_r[slot].astype(F32)).astype(BF16)
        for side in (0, 1):
            keep = (s >= kept) & (par == side)

            @pl.when(keep)
            def _(side=side):
                keep_copy(s, slot, side).start()

            @pl.when(jnp.logical_not(keep))
            def _(side=side):
                own_copy(s, slot, side).start()
        loc_copy(s, slot).start()

    def relay(s):
        slot, par = lax.rem(s, DEPTH), lax.rem(s, 2)
        arrived(ag_rs.at[slot], 2)

        @pl.when(s < kept)
        def _():
            relay_copy(s, par).start()

    def free(s):
        slot, par = lax.rem(s, DEPTH), lax.rem(s, 2)
        arrived(out_sem.at[slot], 6)

        @pl.when((s >= TAIL) & (s < kept + TAIL))
        def _():
            relay_copy(s - TAIL, par).wait()

    actions = {"pair": pair, "own": own, "relay": relay, "free": free}

    def events(t, mask, done):
        out = []
        for e in EVENTS:
            hit = lax.shift_right_logical(mask[e], t) & 1

            @pl.when(hit == 1)
            def _(e=e, c=done[len(out)]):
                actions[e](c)

            out.append(done[len(out)] + hit)
        return tuple(out)

    def state(b):
        return {e: pick(b, masks[e]) for e in EVENTS}, b * steps

    def gu_phase(b, r, exchange=True):
        mask, base = state(b)
        x_copy(b, r).wait()
        if not exchange:
            start_gu(jnp.int32(1), jnp.int32(1))

        def gu_step(t, done):
            slot = lax.rem(base + t, WBUF)
            tile_wait(slot)
            ahead = t + WBUF - 1
            later = lax.rem(base + ahead, WBUF)

            @pl.when(ahead < gu_steps)
            def _():
                start_gu(ahead, later)

            @pl.when(ahead >= gu_steps)
            def _():
                start_dn(ahead - gu_steps, later)

            xb = xv[0:r, :]
            gate = jnp.dot(xb, wv[slot, :, 0:TN], preferred_element_type=F32)
            up = jnp.dot(xb, wv[slot, :, TN:2 * TN], preferred_element_type=F32)
            hv[0:r, pl.ds(pl.multiple_of(t * TN, TN), TN)] = (jax.nn.silu(gate) * up).astype(BF16)
            return events(t, mask, done) if exchange else done

        lax.fori_loop(0, gu_steps, gu_step, tuple(pick(b, starts[e]) for e in EVENTS))

    def dn_phase(b, r):
        units = r // UNIT
        first = pick(b, [v // UNIT for v in row0])
        mask, base = state(b)
        for r2 in sorted(set(BLOCKS)):
            @pl.when(pick(b + 1, [v == r2 for v in BLOCKS]) == 1)
            def _(r2=r2):
                x_copy(b + 1, r2).start()

        def dn_step(t, done):
            g = base + gu_steps + t
            slot = lax.rem(g, WBUF)
            tile_wait(slot)
            ahead = t + WBUF - 1
            later = lax.rem(g + WBUF - 1, WBUF)

            @pl.when(ahead < dn_steps)
            def _():
                start_dn(ahead, later)

            @pl.when((ahead >= dn_steps) & (b + 1 < nb))
            def _():
                start_gu(ahead - dn_steps, later)

            p, j = t // per_piece, lax.rem(t, per_piece)
            c = pl.ds(pl.multiple_of(j * TD, TD), TD)
            term = jnp.dot(hv[0:r, :], wv[slot, 0:hidden, :], preferred_element_type=F32)
            rest = (jnp.dot(hv[0:r, 0:half], wv[slot, hidden:hidden + half, 0:side], preferred_element_type=F32)
                    + jnp.dot(hv[0:r, half:hidden], wv[slot, hidden:hidden + half, side:2 * side], preferred_element_type=F32))
            c0 = pl.ds(pl.multiple_of(j * TD, TN), 2 * TN)
            c1 = pl.ds(pl.multiple_of(j * TD + 2 * TN, TN), side)
            for k in range(units):
                hold[lax.rem(first + k, DEPTH), p, :, c0] = term[k * UNIT:(k + 1) * UNIT, :]
                hold[lax.rem(first + k, DEPTH), p, :, c1] = rest[k * UNIT:(k + 1) * UNIT, :]

            @pl.when(p == 0)
            def _():
                def send(k, _):
                    s = first + k
                    slot, par = lax.rem(s, DEPTH), lax.rem(s, 2)
                    opp_s[slot, :, c] = hold[slot, 0, :, c].astype(BF16)
                    opp_copy(s, slot, par, c).start()
                    return 0
                lax.fori_loop(0, units, send, 0)

            @pl.when((p == 1) | (p == 2))
            def _():
                def send(k, _):
                    s = first + k
                    slot, par = lax.rem(s, DEPTH), lax.rem(s, 2)

                    @pl.when(p == 2 - par)
                    def _():
                        dir_s[slot, :, c] = hold[slot, p, :, c].astype(BF16)
                        dir_copy(s, slot, par, c).start()
                    return 0
                lax.fori_loop(0, units, send, 0)

            return events(gu_steps + t, mask, done)

        lax.fori_loop(0, dn_steps, dn_step, tuple(pick(b, mid[e]) for e in EVENTS))

    def switch(b, phase):
        for r in sorted(set(BLOCKS)):
            @pl.when(pick(b, [v == r for v in BLOCKS]) == 1)
            def _(r=r):
                phase(b, r)

    barrier = pltpu.get_barrier_semaphore()
    for offset in (1, n - 1):
        pl.semaphore_signal(barrier, inc=1, device_id={"tp": at(offset)}, device_id_type=MESH)
    x_copy(jnp.int32(0), BLOCKS[0]).start()
    start_gu(jnp.int32(0), jnp.int32(0))
    gu_phase(jnp.int32(0), BLOCKS[0], exchange=False)
    pl.semaphore_wait(barrier, 2)

    def outer(b, _):
        switch(b, dn_phase)
        switch(b + 1, gu_phase)
        return 0

    lax.fori_loop(0, nb, outer, 0)

    def tail(g, done):
        b = g // steps
        return events(lax.rem(g, steps), {e: pick(b, masks[e]) for e in EVENTS}, done)

    lax.fori_loop(total_steps, last + 1, tail, tuple(jnp.int32(sum(g < total_steps for g in v)) for v in SCHEDULE.values()))


def copy_kernel(n, y_ref, rel_r_ref, rel_l_ref, out_ref, rows_v, units_v, r_sem, w_sem, ur_sem, uw_sem):
    me = lax.axis_index("tp")
    rows, width = y_ref.shape
    piece = width // n
    full = rows - TAIL * UNIT
    jobs = []
    for i in range(full // CHUNK):
        r = pl.ds(i * CHUNK, CHUNK)
        jobs.append((y_ref.at[r, :], rows_v.at[i], out_ref.at[r, :], r_sem.at[i], w_sem.at[i]))
    for i in range(TAIL):
        r = pl.ds(full + i * UNIT, UNIT)
        for k, offset in enumerate((0, 1, n - 1)):
            c = pl.ds(pl.multiple_of(lax.rem(me + offset, n) * piece, piece), piece)
            src = y_ref.at[r, c]
            if offset == n - 1 and i % 2 == 0:
                src = rel_r_ref.at[i // 2]
            if offset == 1 and i % 2 == 1:
                src = rel_l_ref.at[i // 2]
            jobs.append((src, units_v.at[i, k], out_ref.at[r, c], ur_sem.at[i, k], uw_sem.at[i, k]))
    for src, buf, dst, rs, ws in jobs:
        pltpu.make_async_copy(src, buf, rs).start()
    for src, buf, dst, rs, ws in jobs:
        pltpu.make_async_copy(src, buf, rs).wait()
        pltpu.make_async_copy(buf, dst, ws).start()
    for src, buf, dst, rs, ws in jobs:
        pltpu.make_async_copy(buf, dst, ws).wait()


def finish_kernel(n, from_l_ref, from_r_ref, out_in_ref, out_ref, sem):
    me = lax.axis_index("tp")
    rows, width = out_ref.shape
    piece = width // n
    c = pl.ds(pl.multiple_of(lax.rem(me + 2, n) * piece, piece), piece)
    copies = []
    for i in range(TAIL):
        src = (from_l_ref, from_r_ref)[i % 2].at[i // 2]
        copies.append(pltpu.make_async_copy(src, out_ref.at[pl.ds(rows - (TAIL - i) * UNIT, UNIT), c], sem.at[i]))
    for copy in copies:
        copy.start()
    for copy in copies:
        copy.wait()


def solution(mesh):
    n = mesh.shape["tp"]

    def step(x, w_gate, w_up, w_down):
        rows, din = x.shape
        hidden, width = w_down.shape
        piece = width // n
        rmax = max(BLOCKS)
        ring = pltpu.VMEM((DEPTH, UNIT, piece), BF16)
        dma = pltpu.SemaphoreType.DMA
        rel = jax.ShapeDtypeStruct((TAIL // 2, UNIT, piece), BF16)
        anywhere = pl.BlockSpec(memory_space=pl.ANY)
        y, rel_r, rel_l = pl.pallas_call(
            functools.partial(kernel, n),
            out_shape=(jax.ShapeDtypeStruct((rows, width), BF16), rel, rel),
            in_specs=[anywhere] * 4,
            out_specs=(anywhere,) * 3,
            scratch_shapes=[
                pltpu.VMEM((rmax, din), BF16),
                pltpu.VMEM((WBUF, din, 2 * TN), BF16),
                pltpu.VMEM((rmax, hidden), BF16),
                pltpu.VMEM((DEPTH, n, UNIT, piece), F32),
                ring, ring, ring, ring, ring, ring, ring,
                dma, dma((WBUF,)), dma((DEPTH,)), dma((DEPTH,)), dma((DEPTH,)), dma((DEPTH,)),
                dma((DEPTH + TAIL,)), dma((DEPTH + TAIL,)),
            ],
            compiler_params=pltpu.CompilerParams(
                collective_id=0, has_side_effects=True, vmem_limit_bytes=63 * 2**20),
            cost_estimate=pl.CostEstimate(flops=6 * rows * din * hidden, bytes_accessed=7 * 6 * din * hidden, transcendentals=0),
        )(x, w_gate, w_up, w_down)
        from_l = lax.ppermute(rel_r, "tp", [(i, (i + 1) % n) for i in range(n)])
        from_r = lax.ppermute(rel_l, "tp", [(i, (i - 1) % n) for i in range(n)])
        whole = (rows - TAIL * UNIT) // CHUNK
        out = pl.pallas_call(
            functools.partial(copy_kernel, n),
            out_shape=jax.ShapeDtypeStruct((rows, width), BF16),
            in_specs=[anywhere] * 3,
            out_specs=anywhere,
            scratch_shapes=[
                pltpu.VMEM((whole, CHUNK, width), BF16),
                pltpu.VMEM((TAIL, 3, UNIT, piece), BF16),
                dma((whole,)), dma((whole,)), dma((TAIL, 3)), dma((TAIL, 3)),
            ],
            compiler_params=pltpu.CompilerParams(vmem_limit_bytes=32 * 2**20),
            cost_estimate=pl.CostEstimate(flops=10**10, bytes_accessed=4 * rows * width, transcendentals=0),
        )(y, *(pltpu.with_memory_space_constraint(v, pltpu.HBM) for v in (rel_r, rel_l)))
        vmem = pl.BlockSpec(memory_space=pltpu.VMEM)
        from_l = pltpu.with_memory_space_constraint(from_l, pltpu.VMEM)
        from_r = pltpu.with_memory_space_constraint(from_r, pltpu.VMEM)
        return pl.pallas_call(
            functools.partial(finish_kernel, n),
            out_shape=jax.ShapeDtypeStruct((rows, width), BF16),
            in_specs=[vmem, vmem, anywhere],
            out_specs=anywhere,
            input_output_aliases={2: 0},
            scratch_shapes=[dma((TAIL,))],
        )(from_l, from_r, out)

    return jax.shard_map(
        step,
        mesh=mesh,
        in_specs=(P("dp", None), P(None, "tp"), P(None, "tp"), P("tp", None)),
        out_specs=P("dp", None),
        check_vma=False,
    )
```

```python
import functools

import jax
import jax.numpy as jnp
from jax import lax
from jax.experimental import pallas as pl
from jax.experimental.pallas import tpu as pltpu
from jax.sharding import PartitionSpec as P

MESH = pl.DeviceIdType.MESH
F32, BF16 = jnp.float32, jnp.bfloat16

BLOCKS = (128, 128, 128, 128, 128, 128, 128, 128, 128, 128, 128, 128, 128, 128, 128, 128)
UNIT = 32
LAG = 8
MATE = 4
DEPTH = 20
WBUF = 3
TN = 256
TD = 1536
TAIL = 16
CHUNK = 128

SCHEDULE = {
    "pair": [12, 13, 24, 25, 36, 37, 48, 49, 60, 61, 72, 73, 84, 85, 97, 98, 109, 110, 120, 121, 134, 135, 144, 145, 156, 157, 169, 170, 182, 183, 192, 193],
    "own": [16, 17, 28, 30, 40, 42, 53, 55, 65, 67, 77, 80, 90, 92, 102, 104, 115, 117, 127, 128, 139, 141, 152, 153, 164, 165, 175, 176, 186, 187, 194, 195],
    "relay": [20, 24, 32, 36, 45, 48, 57, 60, 69, 72, 82, 84, 94, 97, 106, 109, 119, 123, 131, 134, 143, 147, 155, 160, 168, 172, 179, 182, 190, 192, 196, 197],
    "free": [20, 24, 32, 36, 45, 48, 57, 60, 69, 72, 82, 84, 94, 97, 106, 109, 119, 123, 131, 134, 143, 147, 155, 160, 168, 172, 179, 182, 190, 192, 196, 197],
}
EVENTS = tuple(SCHEDULE)


def pick(index, values):
    total = jnp.int32(0)
    for i, v in enumerate(values):
        if v:
            total = total + jnp.where(index == i, jnp.int32(v), jnp.int32(0))
    return total


def kernel(n, x_ref, wg_ref, wu_ref, wd_ref, y_ref, rel_r_ref, rel_l_ref, xv, wv, hv, hold,
           opp_s, dir_s, sum_s, own_s, opp_r, dir_r, sum_r,
           mate_s, mate_r,
           x_sem, px_ss, px_rs, w_sem, out_sem, opp_rs, own_rs, ag_rs, re_ss, re_rs, mate_ss, mate_rs):
    me = lax.axis_index("tp")
    core = lax.rem(lax.axis_index("dp"), 2)
    mate = lax.axis_index("dp") + 1 - 2 * core
    rows, depth_in = x_ref.shape
    hidden, width = wd_ref.shape[0] // 2, wd_ref.shape[1]
    piece = width // n
    nu = rows // UNIT
    kept = nu - TAIL
    gu_steps, dn_steps = hidden // TN, width // TD
    per_piece = dn_steps // n
    steps = gu_steps + dn_steps
    nb = len(BLOCKS)
    total_steps = nb * steps
    last = max(max(v) for v in SCHEDULE.values())
    windows = max(nb, last // steps + 1)
    masks = {e: [sum(1 << (g % steps) for g in v if g // steps == b) for b in range(windows)] for e, v in SCHEDULE.items()}
    starts = {e: [sum(g // steps < b for g in v) for b in range(windows)] for e, v in SCHEDULE.items()}
    mid = {e: [sum(g // steps < b or (g // steps == b and g % steps < gu_steps) for g in v) for b in range(windows)] for e, v in SCHEDULE.items()}
    row0 = [sum(BLOCKS[:b]) for b in range(nb)]

    def at(offset):
        return lax.rem(me + offset, n)

    def remote(src, dst, ssem, rsem, target):
        return pltpu.make_async_remote_copy(src_ref=src, dst_ref=dst, send_sem=ssem, recv_sem=rsem,
                                            device_id={"tp": target}, device_id_type=MESH)

    def cols(owner):
        return pl.ds(pl.multiple_of(owner * piece, piece), piece)

    def unit_rows(s):
        return pl.ds(pl.multiple_of(s * UNIT, UNIT), UNIT)

    def gu_copies(t, slot):
        c = pl.ds(pl.multiple_of(core * hidden + t * TN, TN), TN)
        return (pltpu.make_async_copy(wg_ref.at[:, c], wv.at[slot, :, 0:TN], w_sem.at[slot]),
                pltpu.make_async_copy(wu_ref.at[:, c], wv.at[slot, :, TN:2 * TN], w_sem.at[slot]))

    third = 2 * TN

    def dn_copies(t, slot):
        p, j = t // per_piece, lax.rem(t, per_piece)
        c = at(pick(p, (2, 1, 3, 0))) * piece + j * TD
        r = pl.ds(pl.multiple_of(core * hidden, TN), hidden)
        return [pltpu.make_async_copy(wd_ref.at[r, pl.ds(pl.multiple_of(c + i * third, TN), third)],
                                      wv.at[slot, i * hidden:(i + 1) * hidden, :], w_sem.at[slot])
                for i in range(TD // third)]

    def start_dn(t, slot):
        for c in dn_copies(t, slot):
            c.start()

    def tile_wait(slot, depth):
        tile = wv.at[slot, 0:depth, :]
        pltpu.make_async_copy(tile, tile, w_sem.at[slot]).wait()

    def start_gu(t, slot):
        for c in gu_copies(t, slot):
            c.start()

    def x_copy(b, r):
        return pltpu.make_async_copy(x_ref.at[pl.ds(pl.multiple_of(pick(b, row0), UNIT), r), :], xv.at[pl.ds(0, r), :], x_sem)

    def push_copy(b, r):
        return pltpu.make_async_remote_copy(
            src_ref=x_ref.at[pl.ds(pl.multiple_of(pick(b, row0), UNIT), r), :], dst_ref=xv.at[pl.ds(r, r), :],
            send_sem=px_ss, recv_sem=px_rs, device_id={"dp": mate}, device_id_type=MESH)

    def mate_copy(b, t, r):
        q = lax.rem(b * dn_steps + t, MATE)
        return pltpu.make_async_remote_copy(
            src_ref=mate_s.at[q, pl.ds(0, r), :], dst_ref=mate_r.at[q, pl.ds(0, r), :],
            send_sem=mate_ss.at[q], recv_sem=mate_rs.at[q], device_id={"dp": mate}, device_id_type=MESH)

    def opp_copy(s, slot, par, c):
        return remote(opp_s.at[slot, :, c], opp_r.at[slot, :, c], out_sem.at[slot], opp_rs.at[slot], at(1 + 2 * par))

    def dir_copy(s, slot, par, c):
        return remote(dir_s.at[slot, :, c], dir_r.at[slot, :, c], out_sem.at[slot], own_rs.at[slot], at(3 - 2 * par))

    def sum_copy(s, slot, par):
        return remote(sum_s.at[slot], sum_r.at[slot], out_sem.at[slot], own_rs.at[slot], at(1 + 2 * par))

    def own_copy(s, slot, side):
        return remote(own_s.at[slot], y_ref.at[unit_rows(s), cols(me)], out_sem.at[slot], ag_rs.at[slot], at(1 + 2 * side))

    def keep_copy(s, slot, side):
        rel = (rel_r_ref, rel_l_ref)[side].at[(s - kept) // 2]
        return remote(own_s.at[slot], rel, out_sem.at[slot], ag_rs.at[slot], at(1 + 2 * side))

    def relay_copy(s, par):
        view = y_ref.at[unit_rows(s), cols(at(3 - 2 * par))]
        k = lax.rem(s, DEPTH + LAG)
        return remote(view, view, re_ss.at[k], re_rs.at[k], at(1 + 2 * par))

    def loc_copy(s, slot):
        return pltpu.make_async_copy(own_s.at[slot], y_ref.at[unit_rows(s), cols(me)], out_sem.at[slot])

    whole = pl.ds(0, piece)

    def arrived(sem, pieces):
        size = hold.at[0, 0:pieces // 2]
        pltpu.make_async_copy(size, size, sem).wait()

    def duo(k):
        return [(2 * k + par, lax.rem(2 * k + par, DEPTH), par) for par in (0, 1)]

    def pair(k):
        for s, slot, par in duo(k):
            opp_copy(s, slot, par, whole).wait_recv()
            sum_s[slot] = (hold[slot, 1 + par] + opp_r[slot].astype(F32)).astype(BF16)
            sum_copy(s, slot, par).start()

    def own(k):
        for s, slot, par in duo(k):
            arrived(own_rs.at[slot], 2)
            own_s[slot] = (hold[slot, 3] + sum_r[slot].astype(F32) + dir_r[slot].astype(F32)).astype(BF16)
            own_copy(s, slot, 1 - par).start()
            loc_copy(s, slot).start()

        @pl.when(2 * k < kept)
        def _():
            for s, slot, par in duo(k):
                own_copy(s, slot, par).start()

        @pl.when(2 * k >= kept)
        def _():
            for s, slot, par in duo(k):
                keep_copy(s, slot, par).start()

    def relay(k):
        for s, slot, par in duo(k):
            arrived(ag_rs.at[slot], 2)

        @pl.when(2 * k < kept)
        def _():
            for s, slot, par in duo(k):
                relay_copy(s, par).start()

    def free(k):
        for s, slot, par in duo(k):
            arrived(out_sem.at[slot], 6)

        @pl.when((2 * k >= LAG) & (2 * k < kept + LAG))
        def _():
            for s, slot, par in duo(k):
                relay_copy(s - LAG, par).wait()

    actions = {"pair": pair, "own": own, "relay": relay, "free": free}

    def events(t, mask, done):
        out = []
        for e in EVENTS:
            hit = lax.shift_right_logical(mask[e], t) & 1

            @pl.when(hit == 1)
            def _(e=e, c=done[len(out)]):
                actions[e](c)

            out.append(done[len(out)] + hit)
        return tuple(out)

    def state(b):
        return {e: pick(b, masks[e]) for e in EVENTS}, b * steps

    def gu_phase(b, r):
        mask, base = state(b)
        x_copy(b, r).wait()

        def hidden_rows(lo, hi, t, slot):
            xb = xv[lo:hi, :]
            gate = jnp.dot(xb, wv[slot, :, 0:TN], preferred_element_type=F32)
            up = jnp.dot(xb, wv[slot, :, TN:2 * TN], preferred_element_type=F32)
            hv[lo:hi, pl.ds(pl.multiple_of(t * TN, TN), TN)] = (jax.nn.silu(gate) * up).astype(BF16)

        @pl.when(b > 0)
        def _():
            push_copy(b, r).wait()

        if r == BLOCKS[0]:
            @pl.when(b == 0)
            def _():
                start_gu(jnp.int32(1), jnp.int32(1))
                tile_wait(jnp.int32(0), depth_in)
                start_gu(jnp.int32(2), jnp.int32(2))
                hidden_rows(0, r, jnp.int32(0), jnp.int32(0))
                push_copy(b, r).wait()
                hidden_rows(r, 2 * r, jnp.int32(0), jnp.int32(0))

        def gu_step(t, done):
            slot = lax.rem(base + t, WBUF)
            tile_wait(slot, depth_in)
            ahead = t + WBUF - 1
            later = lax.rem(base + ahead, WBUF)

            @pl.when(ahead < gu_steps)
            def _():
                start_gu(ahead, later)

            @pl.when(ahead >= gu_steps)
            def _():
                start_dn(ahead - gu_steps, later)

            hidden_rows(0, 2 * r, t, slot)

            @pl.when((t == 0) & (b > 0))
            def _():
                switch(b - 1, lambda b, r: merge(b, dn_steps - 1, r))

            return events(t, mask, done)

        lax.fori_loop(jnp.where(b == 0, 1, 0), gu_steps, gu_step, tuple(pick(b, starts[e]) for e in EVENTS))

    def merge(b, t, r):
        first = pick(b, [v // UNIT for v in row0])
        q = lax.rem(b * dn_steps + t, MATE)
        mate_copy(b, t, r).wait()
        for k in range(r // UNIT):
            s, par = first + k, k % 2
            slot = lax.rem(s, DEPTH)
            both = hold[slot, t] + mate_r[q, k * UNIT:(k + 1) * UNIT, :].astype(F32)
            if t == 0:
                opp_s[slot] = both.astype(BF16)
                opp_copy(s, slot, par, whole).start()
            elif t == 2 - par:
                dir_s[slot] = both.astype(BF16)
                dir_copy(s, slot, par, whole).start()
            else:
                hold[slot, t] = both

    def dn_phase(b, r):
        units = r // UNIT
        first = pick(b, [v // UNIT for v in row0])
        mask, base = state(b)

        done = tuple(pick(b, mid[e]) for e in EVENTS)
        for t in range(dn_steps):
            g = base + gu_steps + t
            slot = lax.rem(g, WBUF)
            tile_wait(slot, dn_steps // n * hidden * TD // (2 * TN))
            ahead = t + WBUF - 1
            later = lax.rem(g + WBUF - 1, WBUF)
            if ahead < dn_steps:
                start_dn(jnp.int32(ahead), later)
            else:
                @pl.when(b + 1 < nb)
                def _(ahead=ahead, later=later):
                    start_gu(jnp.int32(ahead - dn_steps), later)

            q = lax.rem(b * dn_steps + t, MATE)
            for i in range(TD // third):
                term = jnp.dot(hv[0:2 * r, :], wv[slot, i * hidden:(i + 1) * hidden, :], preferred_element_type=F32)
                c = slice(i * third, (i + 1) * third)
                for k in range(units):
                    hold[lax.rem(first + k, DEPTH), t, :, c] = term[k * UNIT:(k + 1) * UNIT, :]
                mate_s[q, 0:r, c] = term[r:2 * r, :].astype(BF16)
            mate_copy(b, t, r).start()
            if t > 0:
                merge(b, t - 1, r)
            if t == 1:
                for r2 in sorted(set(BLOCKS)):
                    @pl.when(pick(b + 1, [v == r2 for v in BLOCKS]) == 1)
                    def _(r2=r2):
                        x_copy(b + 1, r2).start()
                        push_copy(b + 1, r2).start()
            done = events(jnp.int32(gu_steps + t), mask, done)

    def switch(b, phase):
        for r in sorted(set(BLOCKS)):
            @pl.when(pick(b, [v == r for v in BLOCKS]) == 1)
            def _(r=r):
                phase(b, r)

    x_copy(jnp.int32(0), BLOCKS[0]).start()
    start_gu(jnp.int32(0), jnp.int32(0))
    barrier = pltpu.get_barrier_semaphore()
    for other in ({"tp": at(1)}, {"tp": at(n - 1)}, {"dp": mate}):
        pl.semaphore_signal(barrier, inc=1, device_id=other, device_id_type=MESH)
    pl.semaphore_wait(barrier, 3)
    push_copy(jnp.int32(0), BLOCKS[0]).start()

    def outer(b, _):
        switch(b, gu_phase)
        switch(b, dn_phase)
        return 0

    lax.fori_loop(0, nb, outer, 0)
    merge(jnp.int32(nb - 1), dn_steps - 1, BLOCKS[-1])

    def tail(g, done):
        b = g // steps
        return events(lax.rem(g, steps), {e: pick(b, masks[e]) for e in EVENTS}, done)

    lax.fori_loop(total_steps, last + 1, tail, tuple(jnp.int32(sum(g < total_steps for g in v)) for v in SCHEDULE.values()))


def copy_kernel(n, y_ref, rel_r_ref, rel_l_ref, out_ref, rows_v, units_v, r_sem, w_sem, ur_sem, uw_sem):
    me = lax.axis_index("tp")
    rows, width = y_ref.shape
    piece = width // n
    full = rows - TAIL * UNIT
    jobs = []
    for i in range(full // CHUNK):
        r = pl.ds(i * CHUNK, CHUNK)
        jobs.append((y_ref.at[r, :], rows_v.at[i], out_ref.at[r, :], r_sem.at[i], w_sem.at[i]))
    for i in range(TAIL):
        r = pl.ds(full + i * UNIT, UNIT)
        for k, offset in enumerate((0, 1, n - 1)):
            c = pl.ds(pl.multiple_of(lax.rem(me + offset, n) * piece, piece), piece)
            src = y_ref.at[r, c]
            if offset == n - 1 and i % 2 == 0:
                src = rel_r_ref.at[i // 2]
            if offset == 1 and i % 2 == 1:
                src = rel_l_ref.at[i // 2]
            jobs.append((src, units_v.at[i, k], out_ref.at[r, c], ur_sem.at[i, k], uw_sem.at[i, k]))
    for src, buf, dst, rs, ws in jobs:
        pltpu.make_async_copy(src, buf, rs).start()
    for src, buf, dst, rs, ws in jobs:
        pltpu.make_async_copy(src, buf, rs).wait()
        pltpu.make_async_copy(buf, dst, ws).start()
    for src, buf, dst, rs, ws in jobs:
        pltpu.make_async_copy(buf, dst, ws).wait()


def finish_kernel(n, from_l_ref, from_r_ref, out_in_ref, out_ref, sem):
    me = lax.axis_index("tp")
    rows, width = out_ref.shape
    piece = width // n
    c = pl.ds(pl.multiple_of(lax.rem(me + 2, n) * piece, piece), piece)
    copies = []
    for i in range(TAIL):
        src = (from_l_ref, from_r_ref)[i % 2].at[i // 2]
        copies.append(pltpu.make_async_copy(src, out_ref.at[pl.ds(rows - (TAIL - i) * UNIT, UNIT), c], sem.at[i]))
    for copy in copies:
        copy.start()
    for copy in copies:
        copy.wait()


def solution(mesh):
    n = mesh.shape["tp"]

    def step(x, w_gate, w_up, w_down):
        rows, din = x.shape
        hidden, width = w_down.shape
        piece = width // n
        rmax = max(BLOCKS)
        ring = pltpu.VMEM((DEPTH, UNIT, piece), BF16)
        dma = pltpu.SemaphoreType.DMA
        rel = jax.ShapeDtypeStruct((TAIL // 2, UNIT, piece), BF16)
        anywhere = pl.BlockSpec(memory_space=pl.ANY)
        y, rel_r, rel_l = pl.pallas_call(
            functools.partial(kernel, n),
            out_shape=(jax.ShapeDtypeStruct((rows, width), BF16), rel, rel),
            in_specs=[anywhere] * 4,
            out_specs=(anywhere,) * 3,
            scratch_shapes=[
                pltpu.VMEM((2 * rmax, din), BF16),
                pltpu.VMEM((WBUF, din, 2 * TN), BF16),
                pltpu.VMEM((2 * rmax, hidden // 2), BF16),
                pltpu.VMEM((DEPTH, n, UNIT, piece), F32),
                ring, ring, ring, ring, ring, ring, ring,
                pltpu.VMEM((MATE, rmax, TD), BF16), pltpu.VMEM((MATE, rmax, TD), BF16),
                dma, dma, dma, dma((WBUF,)), dma((DEPTH,)), dma((DEPTH,)), dma((DEPTH,)), dma((DEPTH,)),
                dma((DEPTH + LAG,)), dma((DEPTH + LAG,)), dma((MATE,)), dma((MATE,)),
            ],
            compiler_params=pltpu.CompilerParams(
                collective_id=0, has_side_effects=True, vmem_limit_bytes=63 * 2**20),
            cost_estimate=pl.CostEstimate(flops=6 * rows * din * hidden, bytes_accessed=7 * 6 * din * hidden, transcendentals=0),
        )(x, w_gate, w_up, w_down)
        from_l = lax.ppermute(rel_r, "tp", [(i, (i + 1) % n) for i in range(n)])
        from_r = lax.ppermute(rel_l, "tp", [(i, (i - 1) % n) for i in range(n)])
        whole = (rows - TAIL * UNIT) // CHUNK
        out = pl.pallas_call(
            functools.partial(copy_kernel, n),
            out_shape=jax.ShapeDtypeStruct((rows, width), BF16),
            in_specs=[anywhere] * 3,
            out_specs=anywhere,
            scratch_shapes=[
                pltpu.VMEM((whole, CHUNK, width), BF16),
                pltpu.VMEM((TAIL, 3, UNIT, piece), BF16),
                dma((whole,)), dma((whole,)), dma((TAIL, 3)), dma((TAIL, 3)),
            ],
            compiler_params=pltpu.CompilerParams(vmem_limit_bytes=32 * 2**20),
            cost_estimate=pl.CostEstimate(flops=10**10, bytes_accessed=4 * rows * width, transcendentals=0),
        )(y, *(pltpu.with_memory_space_constraint(v, pltpu.HBM) for v in (rel_r, rel_l)))
        vmem = pl.BlockSpec(memory_space=pltpu.VMEM)
        from_l = pltpu.with_memory_space_constraint(from_l, pltpu.VMEM)
        from_r = pltpu.with_memory_space_constraint(from_r, pltpu.VMEM)
        return pl.pallas_call(
            functools.partial(finish_kernel, n),
            out_shape=jax.ShapeDtypeStruct((rows, width), BF16),
            in_specs=[vmem, vmem, anywhere],
            out_specs=anywhere,
            input_output_aliases={2: 0},
            scratch_shapes=[dma((TAIL,))],
        )(from_l, from_r, out)

    return jax.shard_map(
        step,
        mesh=mesh,
        in_specs=(P("dp", None), P(None, "tp"), P(None, "tp"), P("tp", None)),
        out_specs=P("dp", None),
        check_vma=False,
    )
```

```python
import functools

import jax
import jax.numpy as jnp
from jax import lax
from jax.experimental import pallas as pl
from jax.experimental.pallas import tpu as pltpu
from jax.sharding import PartitionSpec as P

MESH = pl.DeviceIdType.MESH
F32, BF16 = jnp.float32, jnp.bfloat16

BLOCKS = (128, 128, 128, 128, 128, 128, 128, 128, 128, 128, 128, 192, 192, 128, 128)
UNIT = 32
LAG = 8
MATE = 4
DEPTH = 20
WBUF = 3
TN = 256
TD = 1536
TAIL = 16
CHUNK = 128

SCHEDULE = {
    "pair": [12, 13, 24, 25, 36, 37, 48, 49, 60, 61, 72, 73, 84, 85, 97, 98, 109, 110, 120, 121, 133, 134, 143, 144, 145, 156, 157, 158, 171, 172, 180, 181],
    "own": [16, 17, 28, 30, 40, 42, 53, 55, 65, 67, 77, 80, 90, 92, 102, 104, 115, 117, 127, 128, 137, 138, 147, 149, 150, 162, 163, 164, 175, 176, 182, 183],
    "relay": [20, 24, 32, 36, 45, 48, 57, 60, 69, 72, 82, 84, 94, 97, 106, 109, 119, 123, 131, 133, 140, 143, 151, 152, 156, 166, 168, 171, 179, 180, 184, 185],
    "free": [20, 24, 32, 36, 45, 48, 57, 60, 69, 72, 82, 84, 94, 97, 106, 109, 119, 123, 131, 133, 140, 143, 151, 152, 156, 166, 168, 171, 179, 180, 184, 185],
}
EVENTS = tuple(SCHEDULE)


def pick(index, values):
    total = jnp.int32(0)
    for i, v in enumerate(values):
        if v:
            total = total + jnp.where(index == i, jnp.int32(v), jnp.int32(0))
    return total


def kernel(n, x_ref, wg_ref, wu_ref, wd_ref, y_ref, rel_r_ref, rel_l_ref, xv, wv, hv, hold,
           opp_s, dir_s, sum_s, own_s, opp_r, dir_r, sum_r,
           mate_s, mate_r,
           x_sem, px_ss, px_rs, w_sem, out_sem, opp_rs, own_rs, ag_rs, re_ss, re_rs, mate_ss, mate_rs):
    me = lax.axis_index("tp")
    core = lax.rem(lax.axis_index("dp"), 2)
    mate = lax.axis_index("dp") + 1 - 2 * core
    rows, depth_in = x_ref.shape
    hidden, width = wd_ref.shape[0] // 2, wd_ref.shape[1]
    piece = width // n
    nu = rows // UNIT
    kept = nu - TAIL
    gu_steps, dn_steps = hidden // TN, width // TD
    per_piece = dn_steps // n
    steps = gu_steps + dn_steps
    nb = len(BLOCKS)
    total_steps = nb * steps
    last = max(max(v) for v in SCHEDULE.values())
    windows = max(nb, last // steps + 1)
    masks = {e: [sum(1 << (g % steps) for g in v if g // steps == b) for b in range(windows)] for e, v in SCHEDULE.items()}
    starts = {e: [sum(g // steps < b for g in v) for b in range(windows)] for e, v in SCHEDULE.items()}
    mid = {e: [sum(g // steps < b or (g // steps == b and g % steps < gu_steps) for g in v) for b in range(windows)] for e, v in SCHEDULE.items()}
    row0 = [sum(BLOCKS[:b]) for b in range(nb)]

    def at(offset):
        return lax.rem(me + offset, n)

    def remote(src, dst, ssem, rsem, target):
        return pltpu.make_async_remote_copy(src_ref=src, dst_ref=dst, send_sem=ssem, recv_sem=rsem,
                                            device_id={"tp": target}, device_id_type=MESH)

    def cols(owner):
        return pl.ds(pl.multiple_of(owner * piece, piece), piece)

    def unit_rows(s):
        return pl.ds(pl.multiple_of(s * UNIT, UNIT), UNIT)

    def gu_copies(t, slot):
        c = pl.ds(pl.multiple_of(core * hidden + t * TN, TN), TN)
        return (pltpu.make_async_copy(wg_ref.at[:, c], wv.at[slot, :, 0:TN], w_sem.at[slot]),
                pltpu.make_async_copy(wu_ref.at[:, c], wv.at[slot, :, TN:2 * TN], w_sem.at[slot]))

    third = 2 * TN

    def dn_copies(t, slot):
        p, j = t // per_piece, lax.rem(t, per_piece)
        c = at(pick(p, (2, 1, 3, 0))) * piece + j * TD
        r = pl.ds(pl.multiple_of(core * hidden, TN), hidden)
        return [pltpu.make_async_copy(wd_ref.at[r, pl.ds(pl.multiple_of(c + i * third, TN), third)],
                                      wv.at[slot, i * hidden:(i + 1) * hidden, :], w_sem.at[slot])
                for i in range(TD // third)]

    def start_dn(t, slot):
        for c in dn_copies(t, slot):
            c.start()

    def tile_wait(slot, depth):
        tile = wv.at[slot, 0:depth, :]
        pltpu.make_async_copy(tile, tile, w_sem.at[slot]).wait()

    def start_gu(t, slot):
        for c in gu_copies(t, slot):
            c.start()

    def x_copy(b, r):
        return pltpu.make_async_copy(x_ref.at[pl.ds(pl.multiple_of(pick(b, row0), UNIT), r), :], xv.at[pl.ds(0, r), :], x_sem)

    def push_copy(b, r):
        return pltpu.make_async_remote_copy(
            src_ref=x_ref.at[pl.ds(pl.multiple_of(pick(b, row0), UNIT), r), :], dst_ref=xv.at[pl.ds(r, r), :],
            send_sem=px_ss, recv_sem=px_rs, device_id={"dp": mate}, device_id_type=MESH)

    def mate_copy(b, t, r):
        q = lax.rem(b * dn_steps + t, MATE)
        return pltpu.make_async_remote_copy(
            src_ref=mate_s.at[q, pl.ds(0, r), :], dst_ref=mate_r.at[q, pl.ds(0, r), :],
            send_sem=mate_ss.at[q], recv_sem=mate_rs.at[q], device_id={"dp": mate}, device_id_type=MESH)

    def opp_copy(s, slot, par, c):
        return remote(opp_s.at[slot, :, c], opp_r.at[slot, :, c], out_sem.at[slot // 2], opp_rs.at[slot // 2], at(1 + 2 * par))

    def dir_copy(s, slot, par, c):
        return remote(dir_s.at[slot, :, c], dir_r.at[slot, :, c], out_sem.at[slot // 2], own_rs.at[slot // 2], at(3 - 2 * par))

    def sum_copy(s, slot, par):
        return remote(sum_s.at[slot], sum_r.at[slot], out_sem.at[slot // 2], own_rs.at[slot // 2], at(1 + 2 * par))

    def own_copy(s, slot, side):
        return remote(own_s.at[slot], y_ref.at[unit_rows(s), cols(me)], out_sem.at[slot // 2], ag_rs.at[slot // 2], at(1 + 2 * side))

    def keep_copy(s, slot, side):
        rel = (rel_r_ref, rel_l_ref)[side].at[(s - kept) // 2]
        return remote(own_s.at[slot], rel, out_sem.at[slot // 2], ag_rs.at[slot // 2], at(1 + 2 * side))

    def relay_copy(s, par):
        view = y_ref.at[unit_rows(s), cols(at(3 - 2 * par))]
        k = lax.rem(s, DEPTH + LAG) // 2
        return remote(view, view, re_ss.at[k], re_rs.at[k], at(1 + 2 * par))

    def loc_copy(s, slot):
        return pltpu.make_async_copy(own_s.at[slot], y_ref.at[unit_rows(s), cols(me)], out_sem.at[slot // 2])

    whole = pl.ds(0, piece)

    def arrived(sem, k, pieces):
        size = hold.at[0:pieces // 2, 0]
        pltpu.make_async_copy(size, size, sem.at[lax.rem(k, DEPTH // 2)]).wait()

    def duo(k):
        return [(2 * k + par, lax.rem(2 * k + par, DEPTH), par) for par in (0, 1)]

    def pair(k):
        arrived(opp_rs, k, 2)
        for s, slot, par in duo(k):
            sum_s[slot] = (hold[slot, 1 + par] + opp_r[slot].astype(F32)).astype(BF16)
            sum_copy(s, slot, par).start()

    def own(k):
        arrived(own_rs, k, 4)
        for s, slot, par in duo(k):
            own_s[slot] = (hold[slot, 3] + sum_r[slot].astype(F32) + dir_r[slot].astype(F32)).astype(BF16)
            own_copy(s, slot, 1 - par).start()
            loc_copy(s, slot).start()

        @pl.when(2 * k < kept)
        def _():
            for s, slot, par in duo(k):
                own_copy(s, slot, par).start()

        @pl.when(2 * k >= kept)
        def _():
            for s, slot, par in duo(k):
                keep_copy(s, slot, par).start()

    def relay(k):
        arrived(ag_rs, k, 4)

        @pl.when(2 * k < kept)
        def _():
            for s, slot, par in duo(k):
                relay_copy(s, par).start()

    def free(k):
        arrived(out_sem, k, 12)

        @pl.when((2 * k >= LAG) & (2 * k < kept + LAG))
        def _():
            i = lax.rem(2 * k - LAG, DEPTH + LAG) // 2
            for sem in (re_ss, re_rs):
                pltpu.make_async_copy(hold.at[0, 0], hold.at[0, 0], sem.at[i]).wait()

    actions = {"pair": pair, "own": own, "relay": relay, "free": free}

    def events(t, mask, done):
        hits = [lax.shift_right_logical(mask[e], t) & 1 for e in EVENTS]

        @pl.when(sum(hits) > 0)
        def _():
            for e, hit, c in zip(EVENTS, hits, done):
                @pl.when(hit == 1)
                def _(e=e, c=c):
                    actions[e](c)

        return tuple(c + hit for c, hit in zip(done, hits))

    def state(b):
        return {e: pick(b, masks[e]) for e in EVENTS}, b * steps

    def gu_phase(b, r):
        mask, base = state(b)
        x_copy(b, r).wait()

        def hidden_rows(lo, hi, t, slot):
            xb = xv[lo:hi, :]
            gate = jnp.dot(xb, wv[slot, :, 0:TN], preferred_element_type=F32)
            up = jnp.dot(xb, wv[slot, :, TN:2 * TN], preferred_element_type=F32)
            hv[lo:hi, pl.ds(pl.multiple_of(t * TN, TN), TN)] = (jax.nn.silu(gate) * up).astype(BF16)

        @pl.when(b > 0)
        def _():
            push_copy(b, r).wait()

        if r == BLOCKS[0]:
            @pl.when(b == 0)
            def _():
                start_gu(jnp.int32(1), jnp.int32(1))
                tile_wait(jnp.int32(0), depth_in)
                start_gu(jnp.int32(2), jnp.int32(2))
                hidden_rows(0, r, jnp.int32(0), jnp.int32(0))
                push_copy(b, r).wait()
                hidden_rows(r, 2 * r, jnp.int32(0), jnp.int32(0))

        def gu_step(t, done):
            slot = lax.rem(base + t, WBUF)
            tile_wait(slot, depth_in)
            ahead = t + WBUF - 1
            later = lax.rem(base + ahead, WBUF)

            @pl.when(ahead < gu_steps)
            def _():
                start_gu(ahead, later)

            @pl.when(ahead >= gu_steps)
            def _():
                start_dn(ahead - gu_steps, later)

            hidden_rows(0, 2 * r, t, slot)

            @pl.when((t == 0) & (b > 0))
            def _():
                switch(b - 1, lambda b, r: merge(b, dn_steps - 1, r))

            return events(t, mask, done)

        lax.fori_loop(jnp.where(b == 0, 1, 0), gu_steps, gu_step, tuple(pick(b, starts[e]) for e in EVENTS))

    def merge(b, t, r):
        first = pick(b, [v // UNIT for v in row0])
        q = lax.rem(b * dn_steps + t, MATE)
        mate_copy(b, t, r).wait()
        for k in range(r // UNIT):
            s, par = first + k, k % 2
            slot = lax.rem(s, DEPTH)
            both = hold[slot, t] + mate_r[q, k * UNIT:(k + 1) * UNIT, :].astype(F32)
            if t == 0:
                opp_s[slot] = both.astype(BF16)
                opp_copy(s, slot, par, whole).start()
            elif t == 2 - par:
                dir_s[slot] = both.astype(BF16)
                dir_copy(s, slot, par, whole).start()
            else:
                hold[slot, t] = both

    def dn_phase(b, r):
        units = r // UNIT
        first = pick(b, [v // UNIT for v in row0])
        mask, base = state(b)

        def dn_step(t, done):
            g = base + gu_steps + t
            slot = lax.rem(g, WBUF)
            tile_wait(slot, dn_steps // n * hidden * TD // (2 * TN))
            ahead = t + WBUF - 1
            later = lax.rem(g + WBUF - 1, WBUF)

            @pl.when(ahead < dn_steps)
            def _():
                start_dn(ahead, later)

            @pl.when((ahead >= dn_steps) & (b + 1 < nb))
            def _():
                start_gu(ahead - dn_steps, later)

            q = lax.rem(b * dn_steps + t, MATE)
            for i in range(TD // third):
                term = jnp.dot(hv[0:2 * r, :], wv[slot, i * hidden:(i + 1) * hidden, :], preferred_element_type=F32)
                c = slice(i * third, (i + 1) * third)
                for k in range(units):
                    hold[lax.rem(first + k, DEPTH), t, :, c] = term[k * UNIT:(k + 1) * UNIT, :]
                mate_s[q, 0:r, c] = term[r:2 * r, :].astype(BF16)
            mate_copy(b, t, r).start()
            for done_tile in range(dn_steps - 1):
                @pl.when(t == done_tile + 1)
                def _(done_tile=done_tile):
                    merge(b, done_tile, r)
                    if done_tile == 0:
                        for r2 in sorted(set(BLOCKS)):
                            @pl.when(pick(b + 1, [v == r2 for v in BLOCKS]) == 1)
                            def _(r2=r2):
                                x_copy(b + 1, r2).start()
                                push_copy(b + 1, r2).start()
            return events(gu_steps + t, mask, done)

        lax.fori_loop(0, dn_steps, dn_step, tuple(pick(b, mid[e]) for e in EVENTS))

    def switch(b, phase):
        for r in sorted(set(BLOCKS)):
            @pl.when(pick(b, [v == r for v in BLOCKS]) == 1)
            def _(r=r):
                phase(b, r)

    x_copy(jnp.int32(0), BLOCKS[0]).start()
    start_gu(jnp.int32(0), jnp.int32(0))
    barrier = pltpu.get_barrier_semaphore()
    for other in ({"tp": at(1)}, {"tp": at(n - 1)}, {"dp": mate}):
        pl.semaphore_signal(barrier, inc=1, device_id=other, device_id_type=MESH)
    pl.semaphore_wait(barrier, 3)
    push_copy(jnp.int32(0), BLOCKS[0]).start()

    def outer(b, _):
        switch(b, gu_phase)
        switch(b, dn_phase)
        return 0

    lax.fori_loop(0, nb, outer, 0)
    merge(jnp.int32(nb - 1), dn_steps - 1, BLOCKS[-1])

    def tail(g, done):
        b = g // steps
        return events(lax.rem(g, steps), {e: pick(b, masks[e]) for e in EVENTS}, done)

    lax.fori_loop(total_steps, last + 1, tail, tuple(jnp.int32(sum(g < total_steps for g in v)) for v in SCHEDULE.values()))


def copy_kernel(n, y_ref, rel_r_ref, rel_l_ref, out_ref, rows_v, units_v, r_sem, w_sem, ur_sem, uw_sem):
    me = lax.axis_index("tp")
    rows, width = y_ref.shape
    piece = width // n
    full = rows - TAIL * UNIT
    jobs = []
    for i in range(full // CHUNK):
        r = pl.ds(i * CHUNK, CHUNK)
        jobs.append((y_ref.at[r, :], rows_v.at[i], out_ref.at[r, :], r_sem.at[i], w_sem.at[i]))
    for i in range(TAIL):
        r = pl.ds(full + i * UNIT, UNIT)
        for k, offset in enumerate((0, 1, n - 1)):
            c = pl.ds(pl.multiple_of(lax.rem(me + offset, n) * piece, piece), piece)
            src = y_ref.at[r, c]
            if offset == n - 1 and i % 2 == 0:
                src = rel_r_ref.at[i // 2]
            if offset == 1 and i % 2 == 1:
                src = rel_l_ref.at[i // 2]
            jobs.append((src, units_v.at[i, k], out_ref.at[r, c], ur_sem.at[i, k], uw_sem.at[i, k]))
    for src, buf, dst, rs, ws in jobs:
        pltpu.make_async_copy(src, buf, rs).start()
    for src, buf, dst, rs, ws in jobs:
        pltpu.make_async_copy(src, buf, rs).wait()
        pltpu.make_async_copy(buf, dst, ws).start()
    for src, buf, dst, rs, ws in jobs:
        pltpu.make_async_copy(buf, dst, ws).wait()


def finish_kernel(n, from_l_ref, from_r_ref, out_in_ref, out_ref, sem):
    me = lax.axis_index("tp")
    rows, width = out_ref.shape
    piece = width // n
    c = pl.ds(pl.multiple_of(lax.rem(me + 2, n) * piece, piece), piece)
    copies = []
    for i in range(TAIL):
        src = (from_l_ref, from_r_ref)[i % 2].at[i // 2]
        copies.append(pltpu.make_async_copy(src, out_ref.at[pl.ds(rows - (TAIL - i) * UNIT, UNIT), c], sem.at[i]))
    for copy in copies:
        copy.start()
    for copy in copies:
        copy.wait()


def solution(mesh):
    n = mesh.shape["tp"]

    def step(x, w_gate, w_up, w_down):
        rows, din = x.shape
        hidden, width = w_down.shape
        piece = width // n
        rmax = max(BLOCKS)
        ring = pltpu.VMEM((DEPTH, UNIT, piece), BF16)
        dma = pltpu.SemaphoreType.DMA
        rel = jax.ShapeDtypeStruct((TAIL // 2, UNIT, piece), BF16)
        anywhere = pl.BlockSpec(memory_space=pl.ANY)
        y, rel_r, rel_l = pl.pallas_call(
            functools.partial(kernel, n),
            out_shape=(jax.ShapeDtypeStruct((rows, width), BF16), rel, rel),
            in_specs=[anywhere] * 4,
            out_specs=(anywhere,) * 3,
            scratch_shapes=[
                pltpu.VMEM((2 * rmax, din), BF16),
                pltpu.VMEM((WBUF, din, 2 * TN), BF16),
                pltpu.VMEM((2 * rmax, hidden // 2), BF16),
                pltpu.VMEM((DEPTH, n, UNIT, piece), F32),
                ring, ring, ring, ring, ring, ring, ring,
                pltpu.VMEM((MATE, rmax, TD), BF16), pltpu.VMEM((MATE, rmax, TD), BF16),
                dma, dma, dma, dma((WBUF,)), dma((DEPTH // 2,)), dma((DEPTH // 2,)), dma((DEPTH // 2,)), dma((DEPTH // 2,)),
                dma(((DEPTH + LAG) // 2,)), dma(((DEPTH + LAG) // 2,)), dma((MATE + 2,)), dma((MATE + 2,)),
            ],
            compiler_params=pltpu.CompilerParams(
                collective_id=0, has_side_effects=True, vmem_limit_bytes=63 * 2**20),
            cost_estimate=pl.CostEstimate(flops=6 * rows * din * hidden, bytes_accessed=7 * 6 * din * hidden, transcendentals=0),
        )(x, w_gate, w_up, w_down)
        from_l = lax.ppermute(rel_r, "tp", [(i, (i + 1) % n) for i in range(n)])
        from_r = lax.ppermute(rel_l, "tp", [(i, (i - 1) % n) for i in range(n)])
        whole = (rows - TAIL * UNIT) // CHUNK
        out = pl.pallas_call(
            functools.partial(copy_kernel, n),
            out_shape=jax.ShapeDtypeStruct((rows, width), BF16),
            in_specs=[anywhere] * 3,
            out_specs=anywhere,
            scratch_shapes=[
                pltpu.VMEM((whole, CHUNK, width), BF16),
                pltpu.VMEM((TAIL, 3, UNIT, piece), BF16),
                dma((whole,)), dma((whole,)), dma((TAIL, 3)), dma((TAIL, 3)),
            ],
            compiler_params=pltpu.CompilerParams(vmem_limit_bytes=32 * 2**20),
            cost_estimate=pl.CostEstimate(flops=10**10, bytes_accessed=4 * rows * width, transcendentals=0),
        )(y, *(pltpu.with_memory_space_constraint(v, pltpu.HBM) for v in (rel_r, rel_l)))
        vmem = pl.BlockSpec(memory_space=pltpu.VMEM)
        from_l = pltpu.with_memory_space_constraint(from_l, pltpu.VMEM)
        from_r = pltpu.with_memory_space_constraint(from_r, pltpu.VMEM)
        return pl.pallas_call(
            functools.partial(finish_kernel, n),
            out_shape=jax.ShapeDtypeStruct((rows, width), BF16),
            in_specs=[vmem, vmem, anywhere],
            out_specs=anywhere,
            input_output_aliases={2: 0},
            scratch_shapes=[dma((TAIL,))],
        )(from_l, from_r, out)

    return jax.shard_map(
        step,
        mesh=mesh,
        in_specs=(P("dp", None), P(None, "tp"), P(None, "tp"), P("tp", None)),
        out_specs=P("dp", None),
        check_vma=False,
    )
```

```python
import functools

import jax
import jax.numpy as jnp
from jax import lax
from jax.experimental import pallas as pl
from jax.experimental.pallas import tpu as pltpu
from jax.sharding import PartitionSpec as P

MESH = pl.DeviceIdType.MESH
F32, BF16 = jnp.float32, jnp.bfloat16

BLOCKS = (128, 128, 128, 128, 128, 128, 128, 128, 128, 128, 128, 192, 192, 128, 128)
UNIT = 32
LAG = 8
MATE = 4
DEPTH = 20
WBUF = 3
TN = 256
TD = 1536
TAIL = 16
CHUNK = 128

SCHEDULE = {
    "pair": [12, 13, 24, 25, 36, 37, 48, 49, 61, 62, 72, 73, 86, 87, 97, 98, 109, 110, 120, 121, 132, 133, 144, 145, 146, 156, 157, 158, 168, 169, 180, 181],
    "own": [16, 17, 28, 31, 41, 43, 54, 56, 66, 69, 79, 80, 92, 94, 104, 105, 117, 118, 129, 130, 138, 139, 149, 150, 151, 165, 166, 167, 179, 180, 182, 183],
    "relay": [20, 24, 33, 36, 45, 48, 58, 61, 71, 75, 83, 86, 96, 102, 108, 113, 123, 127, 134, 137, 142, 144, 153, 154, 183, 184, 185, 186, 187, 188, 189, 190],
    "free": [20, 24, 33, 36, 45, 48, 58, 61, 71, 75, 83, 86, 96, 102, 108, 113, 123, 127, 134, 137, 142, 144, 153, 154, 183, 184, 185, 186, 187, 188, 189, 190],
}
EVENTS = tuple(SCHEDULE)


def pick(index, values):
    total = jnp.int32(0)
    for i, v in enumerate(values):
        if v:
            total = total + jnp.where(index == i, jnp.int32(v), jnp.int32(0))
    return total


def kernel(n, x_ref, wg_ref, wu_ref, wd_ref, y_ref, rel_r_ref, rel_l_ref, xv, wv, hv, hold,
           opp_s, dir_s, sum_s, own_s, opp_r, dir_r, sum_r,
           mate_s, mate_r,
           x_sem, px_ss, px_rs, w_sem, out_sem, opp_rs, own_rs, ag_rs, re_ss, re_rs, mate_ss, mate_rs):
    me = lax.axis_index("tp")
    core = lax.rem(lax.axis_index("dp"), 2)
    mate = lax.axis_index("dp") + 1 - 2 * core
    rows, depth_in = x_ref.shape
    hidden, width = wd_ref.shape[0] // 2, wd_ref.shape[1]
    piece = width // n
    nu = rows // UNIT
    kept = nu - TAIL
    gu_steps, dn_steps = hidden // TN, width // TD
    per_piece = dn_steps // n
    steps = gu_steps + dn_steps
    nb = len(BLOCKS)
    total_steps = nb * steps
    last = max(max(v) for v in SCHEDULE.values())
    windows = max(nb, last // steps + 1)
    masks = {e: [sum(1 << (g % steps) for g in v if g // steps == b) for b in range(windows)] for e, v in SCHEDULE.items()}
    starts = {e: [sum(g // steps < b for g in v) for b in range(windows)] for e, v in SCHEDULE.items()}
    mid = {e: [sum(g // steps < b or (g // steps == b and g % steps < gu_steps) for g in v) for b in range(windows)] for e, v in SCHEDULE.items()}
    row0 = [sum(BLOCKS[:b]) for b in range(nb)]

    def at(offset):
        return lax.rem(me + offset, n)

    def remote(src, dst, ssem, rsem, target):
        return pltpu.make_async_remote_copy(src_ref=src, dst_ref=dst, send_sem=ssem, recv_sem=rsem,
                                            device_id={"tp": target}, device_id_type=MESH)

    def cols(owner):
        return pl.ds(pl.multiple_of(owner * piece, piece), piece)

    def unit_rows(s):
        return pl.ds(pl.multiple_of(s * UNIT, UNIT), UNIT)

    def gu_copies(t, slot):
        c = pl.ds(pl.multiple_of(core * hidden + t * TN, TN), TN)
        return (pltpu.make_async_copy(wg_ref.at[:, c], wv.at[slot, :, 0:TN], w_sem.at[slot]),
                pltpu.make_async_copy(wu_ref.at[:, c], wv.at[slot, :, TN:2 * TN], w_sem.at[slot]))

    third = 2 * TN

    def dn_copies(t, slot):
        p, j = t // per_piece, lax.rem(t, per_piece)
        c = at(pick(p, (2, 1, 3, 0))) * piece + j * TD
        r = pl.ds(pl.multiple_of(core * hidden, TN), hidden)
        return [pltpu.make_async_copy(wd_ref.at[r, pl.ds(pl.multiple_of(c + i * third, TN), third)],
                                      wv.at[slot, i * hidden:(i + 1) * hidden, :], w_sem.at[slot])
                for i in range(TD // third)]

    def start_dn(t, slot):
        for c in dn_copies(t, slot):
            c.start()

    def tile_wait(slot, depth):
        tile = wv.at[slot, 0:depth, :]
        pltpu.make_async_copy(tile, tile, w_sem.at[slot]).wait()

    def start_gu(t, slot):
        for c in gu_copies(t, slot):
            c.start()

    def x_copy(b, r):
        return pltpu.make_async_copy(x_ref.at[pl.ds(pl.multiple_of(pick(b, row0), UNIT), r), :], xv.at[pl.ds(0, r), :], x_sem)

    def push_copy(b, r):
        return pltpu.make_async_remote_copy(
            src_ref=x_ref.at[pl.ds(pl.multiple_of(pick(b, row0), UNIT), r), :], dst_ref=xv.at[pl.ds(r, r), :],
            send_sem=px_ss, recv_sem=px_rs, device_id={"dp": mate}, device_id_type=MESH)

    def mate_copy(b, t, r):
        q = lax.rem(b * dn_steps + t, MATE)
        return pltpu.make_async_remote_copy(
            src_ref=mate_s.at[q, pl.ds(0, r), :], dst_ref=mate_r.at[q, pl.ds(0, r), :],
            send_sem=mate_ss.at[q], recv_sem=mate_rs.at[q], device_id={"dp": mate}, device_id_type=MESH)

    def opp_copy(s, slot, par, c):
        return remote(opp_s.at[slot, :, c], opp_r.at[slot, :, c], out_sem.at[slot // 2], opp_rs.at[slot // 2], at(1 + 2 * par))

    def dir_copy(s, slot, par, c):
        return remote(dir_s.at[slot, :, c], dir_r.at[slot, :, c], out_sem.at[slot // 2], own_rs.at[slot // 2], at(3 - 2 * par))

    def sum_copy(s, slot, par):
        return remote(sum_s.at[slot], sum_r.at[slot], out_sem.at[slot // 2], own_rs.at[slot // 2], at(1 + 2 * par))

    def own_copy(s, slot, side):
        return remote(own_s.at[slot], y_ref.at[unit_rows(s), cols(me)], out_sem.at[slot // 2], ag_rs.at[slot // 2], at(1 + 2 * side))

    def keep_copy(s, slot, side):
        rel = (rel_r_ref, rel_l_ref)[side].at[(s - kept) // 2]
        return remote(own_s.at[slot], rel, out_sem.at[slot // 2], ag_rs.at[slot // 2], at(1 + 2 * side))

    def relay_copy(s, par):
        view = y_ref.at[unit_rows(s), cols(at(3 - 2 * par))]
        k = lax.rem(s, DEPTH + LAG) // 2
        return remote(view, view, re_ss.at[k], re_rs.at[k], at(1 + 2 * par))

    def loc_copy(s, slot):
        return pltpu.make_async_copy(own_s.at[slot], y_ref.at[unit_rows(s), cols(me)], out_sem.at[slot // 2])

    whole = pl.ds(0, piece)

    def arrived(sem, k, pieces):
        size = hold.at[0:pieces // 2, 0]
        pltpu.make_async_copy(size, size, sem.at[lax.rem(k, DEPTH // 2)]).wait()

    def duo(k):
        return [(2 * k + par, lax.rem(2 * k + par, DEPTH), par) for par in (0, 1)]

    def pair(k):
        arrived(opp_rs, k, 2)
        for s, slot, par in duo(k):
            sum_s[slot] = (hold[slot, 1 + par] + opp_r[slot].astype(F32)).astype(BF16)
            sum_copy(s, slot, par).start()

    def own(k):
        arrived(own_rs, k, 4)
        for s, slot, par in duo(k):
            own_s[slot] = (hold[slot, 3] + sum_r[slot].astype(F32) + dir_r[slot].astype(F32)).astype(BF16)
            own_copy(s, slot, 1 - par).start()
            loc_copy(s, slot).start()

        @pl.when(2 * k < kept)
        def _():
            for s, slot, par in duo(k):
                own_copy(s, slot, par).start()

        @pl.when(2 * k >= kept)
        def _():
            for s, slot, par in duo(k):
                keep_copy(s, slot, par).start()

    def relay(k):
        arrived(ag_rs, k, 4)

        @pl.when(2 * k < kept)
        def _():
            for s, slot, par in duo(k):
                relay_copy(s, par).start()

    def free(k):
        arrived(out_sem, k, 12)

        @pl.when((2 * k >= LAG) & (2 * k < kept + LAG))
        def _():
            i = lax.rem(2 * k - LAG, DEPTH + LAG) // 2
            for sem in (re_ss, re_rs):
                pltpu.make_async_copy(hold.at[0, 0], hold.at[0, 0], sem.at[i]).wait()

    actions = {"pair": pair, "own": own, "relay": relay, "free": free}

    def events(t, mask, done):
        hits = [lax.shift_right_logical(mask[e], t) & 1 for e in EVENTS]

        @pl.when(sum(hits) > 0)
        def _():
            for e, hit, c in zip(EVENTS, hits, done):
                @pl.when(hit == 1)
                def _(e=e, c=c):
                    actions[e](c)

        return tuple(c + hit for c, hit in zip(done, hits))

    def state(b):
        return {e: pick(b, masks[e]) for e in EVENTS}, b * steps

    def gu_phase(b, r):
        mask, base = state(b)
        x_copy(b, r).wait()

        def hidden_rows(lo, hi, t, slot):
            xb = xv[lo:hi, :]
            gate = jnp.dot(xb, wv[slot, :, 0:TN], preferred_element_type=F32)
            up = jnp.dot(xb, wv[slot, :, TN:2 * TN], preferred_element_type=F32)
            hv[lo:hi, pl.ds(pl.multiple_of(t * TN, TN), TN)] = (jax.nn.silu(gate) * up).astype(BF16)

        @pl.when(b > 0)
        def _():
            push_copy(b, r).wait()

        if r == BLOCKS[0]:
            @pl.when(b == 0)
            def _():
                start_gu(jnp.int32(1), jnp.int32(1))
                tile_wait(jnp.int32(0), depth_in)
                start_gu(jnp.int32(2), jnp.int32(2))
                hidden_rows(0, r, jnp.int32(0), jnp.int32(0))
                push_copy(b, r).wait()
                hidden_rows(r, 2 * r, jnp.int32(0), jnp.int32(0))

        def gu_step(t, done):
            slot = lax.rem(base + t, WBUF)
            tile_wait(slot, depth_in)
            ahead = t + WBUF - 1
            later = lax.rem(base + ahead, WBUF)

            @pl.when(ahead < gu_steps)
            def _():
                start_gu(ahead, later)

            @pl.when(ahead >= gu_steps)
            def _():
                start_dn(ahead - gu_steps, later)

            hidden_rows(0, 2 * r, t, slot)

            @pl.when((t == 0) & (b > 0))
            def _():
                switch(b - 1, lambda b, r: merge(b, dn_steps - 1, r))

            return events(t, mask, done)

        lax.fori_loop(jnp.where(b == 0, 1, 0), gu_steps, gu_step, tuple(pick(b, starts[e]) for e in EVENTS))

    def merge(b, t, r):
        first = pick(b, [v // UNIT for v in row0])
        q = lax.rem(b * dn_steps + t, MATE)
        mate_copy(b, t, r).wait()
        for k in range(r // UNIT):
            s, par = first + k, k % 2
            slot = lax.rem(s, DEPTH)
            both = hold[slot, t] + mate_r[q, k * UNIT:(k + 1) * UNIT, :].astype(F32)
            if t == 0:
                opp_s[slot] = both.astype(BF16)
                opp_copy(s, slot, par, whole).start()
            elif t == 2 - par:
                dir_s[slot] = both.astype(BF16)
                dir_copy(s, slot, par, whole).start()
            else:
                hold[slot, t] = both

    def dn_phase(b, r):
        units = r // UNIT
        first = pick(b, [v // UNIT for v in row0])
        mask, base = state(b)

        def dn_step(t, done):
            g = base + gu_steps + t
            slot = lax.rem(g, WBUF)
            tile_wait(slot, dn_steps // n * hidden * TD // (2 * TN))
            ahead = t + WBUF - 1
            later = lax.rem(g + WBUF - 1, WBUF)

            @pl.when(ahead < dn_steps)
            def _():
                start_dn(ahead, later)

            @pl.when((ahead >= dn_steps) & (b + 1 < nb))
            def _():
                start_gu(ahead - dn_steps, later)

            q = lax.rem(b * dn_steps + t, MATE)
            for i in range(TD // third):
                term = jnp.dot(hv[0:2 * r, :], wv[slot, i * hidden:(i + 1) * hidden, :], preferred_element_type=F32)
                c = slice(i * third, (i + 1) * third)
                for k in range(units):
                    hold[lax.rem(first + k, DEPTH), t, :, c] = term[k * UNIT:(k + 1) * UNIT, :]
                mate_s[q, 0:r, c] = term[r:2 * r, :].astype(BF16)
            mate_copy(b, t, r).start()
            for done_tile in range(dn_steps - 1):
                @pl.when(t == done_tile + 1)
                def _(done_tile=done_tile):
                    merge(b, done_tile, r)
                    if done_tile == 0:
                        for r2 in sorted(set(BLOCKS)):
                            @pl.when(pick(b + 1, [v == r2 for v in BLOCKS]) == 1)
                            def _(r2=r2):
                                x_copy(b + 1, r2).start()
                                push_copy(b + 1, r2).start()
            return events(gu_steps + t, mask, done)

        lax.fori_loop(0, dn_steps, dn_step, tuple(pick(b, mid[e]) for e in EVENTS))

    def switch(b, phase):
        for r in sorted(set(BLOCKS)):
            @pl.when(pick(b, [v == r for v in BLOCKS]) == 1)
            def _(r=r):
                phase(b, r)

    x_copy(jnp.int32(0), BLOCKS[0]).start()
    start_gu(jnp.int32(0), jnp.int32(0))
    barrier = pltpu.get_barrier_semaphore()
    for other in ({"tp": at(1)}, {"tp": at(n - 1)}, {"dp": mate}):
        pl.semaphore_signal(barrier, inc=1, device_id=other, device_id_type=MESH)
    pl.semaphore_wait(barrier, 3)
    push_copy(jnp.int32(0), BLOCKS[0]).start()

    def outer(b, _):
        switch(b, gu_phase)
        switch(b, dn_phase)
        return 0

    lax.fori_loop(0, nb, outer, 0)
    merge(jnp.int32(nb - 1), dn_steps - 1, BLOCKS[-1])

    def tail(g, done):
        b = g // steps
        return events(lax.rem(g, steps), {e: pick(b, masks[e]) for e in EVENTS}, done)

    lax.fori_loop(total_steps, last + 1, tail, tuple(jnp.int32(sum(g < total_steps for g in v)) for v in SCHEDULE.values()))


def copy_kernel(n, y_ref, rel_r_ref, rel_l_ref, out_ref, rows_v, units_v, r_sem, w_sem, ur_sem, uw_sem):
    me = lax.axis_index("tp")
    rows, width = y_ref.shape
    piece = width // n
    full = rows - TAIL * UNIT
    jobs = []
    for i in range(full // CHUNK):
        r = pl.ds(i * CHUNK, CHUNK)
        jobs.append((y_ref.at[r, :], rows_v.at[i], out_ref.at[r, :], r_sem.at[i], w_sem.at[i]))
    for i in range(TAIL):
        r = pl.ds(full + i * UNIT, UNIT)
        for k, offset in enumerate((0, 1, n - 1)):
            c = pl.ds(pl.multiple_of(lax.rem(me + offset, n) * piece, piece), piece)
            src = y_ref.at[r, c]
            if offset == n - 1 and i % 2 == 0:
                src = rel_r_ref.at[i // 2]
            if offset == 1 and i % 2 == 1:
                src = rel_l_ref.at[i // 2]
            jobs.append((src, units_v.at[i, k], out_ref.at[r, c], ur_sem.at[i, k], uw_sem.at[i, k]))
    for src, buf, dst, rs, ws in jobs:
        pltpu.make_async_copy(src, buf, rs).start()
    for src, buf, dst, rs, ws in jobs:
        pltpu.make_async_copy(src, buf, rs).wait()
        pltpu.make_async_copy(buf, dst, ws).start()
    for src, buf, dst, rs, ws in jobs:
        pltpu.make_async_copy(buf, dst, ws).wait()


def finish_kernel(n, from_l_ref, from_r_ref, out_in_ref, out_ref, sem):
    me = lax.axis_index("tp")
    rows, width = out_ref.shape
    piece = width // n
    c = pl.ds(pl.multiple_of(lax.rem(me + 2, n) * piece, piece), piece)
    copies = []
    for i in range(TAIL):
        src = (from_l_ref, from_r_ref)[i % 2].at[i // 2]
        copies.append(pltpu.make_async_copy(src, out_ref.at[pl.ds(rows - (TAIL - i) * UNIT, UNIT), c], sem.at[i]))
    for copy in copies:
        copy.start()
    for copy in copies:
        copy.wait()


def solution(mesh):
    n = mesh.shape["tp"]

    def step(x, w_gate, w_up, w_down):
        rows, din = x.shape
        hidden, width = w_down.shape
        piece = width // n
        rmax = max(BLOCKS)
        ring = pltpu.VMEM((DEPTH, UNIT, piece), BF16)
        dma = pltpu.SemaphoreType.DMA
        rel = jax.ShapeDtypeStruct((TAIL // 2, UNIT, piece), BF16)
        anywhere = pl.BlockSpec(memory_space=pl.ANY)
        y, rel_r, rel_l = pl.pallas_call(
            functools.partial(kernel, n),
            out_shape=(jax.ShapeDtypeStruct((rows, width), BF16), rel, rel),
            in_specs=[anywhere] * 4,
            out_specs=(anywhere,) * 3,
            scratch_shapes=[
                pltpu.VMEM((2 * rmax, din), BF16),
                pltpu.VMEM((WBUF, din, 2 * TN), BF16),
                pltpu.VMEM((2 * rmax, hidden // 2), BF16),
                pltpu.VMEM((DEPTH, n, UNIT, piece), F32),
                ring, ring, ring, ring, ring, ring, ring,
                pltpu.VMEM((MATE, rmax, TD), BF16), pltpu.VMEM((MATE, rmax, TD), BF16),
                dma, dma, dma, dma((WBUF,)), dma((DEPTH // 2,)), dma((DEPTH // 2,)), dma((DEPTH // 2,)), dma((DEPTH // 2,)),
                dma(((DEPTH + LAG) // 2,)), dma(((DEPTH + LAG) // 2,)), dma((MATE + 2,)), dma((MATE + 2,)),
            ],
            compiler_params=pltpu.CompilerParams(
                collective_id=0, has_side_effects=True, vmem_limit_bytes=63 * 2**20),
            cost_estimate=pl.CostEstimate(flops=6 * rows * din * hidden, bytes_accessed=7 * 6 * din * hidden, transcendentals=0),
        )(x, w_gate, w_up, w_down)
        from_l = lax.ppermute(rel_r, "tp", [(i, (i + 1) % n) for i in range(n)])
        from_r = lax.ppermute(rel_l, "tp", [(i, (i - 1) % n) for i in range(n)])
        whole = (rows - TAIL * UNIT) // CHUNK
        out = pl.pallas_call(
            functools.partial(copy_kernel, n),
            out_shape=jax.ShapeDtypeStruct((rows, width), BF16),
            in_specs=[anywhere] * 3,
            out_specs=anywhere,
            scratch_shapes=[
                pltpu.VMEM((whole, CHUNK, width), BF16),
                pltpu.VMEM((TAIL, 3, UNIT, piece), BF16),
                dma((whole,)), dma((whole,)), dma((TAIL, 3)), dma((TAIL, 3)),
            ],
            compiler_params=pltpu.CompilerParams(vmem_limit_bytes=32 * 2**20),
            cost_estimate=pl.CostEstimate(flops=10**10, bytes_accessed=4 * rows * width, transcendentals=0),
        )(y, *(pltpu.with_memory_space_constraint(v, pltpu.HBM) for v in (rel_r, rel_l)))
        vmem = pl.BlockSpec(memory_space=pltpu.VMEM)
        from_l = pltpu.with_memory_space_constraint(from_l, pltpu.VMEM)
        from_r = pltpu.with_memory_space_constraint(from_r, pltpu.VMEM)
        return pl.pallas_call(
            functools.partial(finish_kernel, n),
            out_shape=jax.ShapeDtypeStruct((rows, width), BF16),
            in_specs=[vmem, vmem, anywhere],
            out_specs=anywhere,
            input_output_aliases={2: 0},
            scratch_shapes=[dma((TAIL,))],
        )(from_l, from_r, out)

    return jax.shard_map(
        step,
        mesh=mesh,
        in_specs=(P("dp", None), P(None, "tp"), P(None, "tp"), P("tp", None)),
        out_specs=P("dp", None),
        check_vma=False,
    )
```

```python
import functools

import jax
import jax.numpy as jnp
from jax import lax
from jax.experimental import pallas as pl
from jax.experimental.pallas import tpu as pltpu
from jax.sharding import PartitionSpec as P

MESH = pl.DeviceIdType.MESH
F32, BF16 = jnp.float32, jnp.bfloat16

BLOCKS = (128, 128, 128, 128, 128, 128, 128, 128, 128, 128, 128, 192, 192, 128, 128)
UNIT = 32
LAG = 8
MATE = 4
DEPTH = 20
WBUF = 3
TN = 256
TD = 1536
TAIL = 16
CHUNK = 128

SCHEDULE = {
    "pair": [12, 13, 24, 25, 36, 37, 48, 49, 61, 62, 72, 73, 86, 87, 97, 98, 109, 110, 120, 121, 132, 133, 144, 145, 146, 156, 157, 158, 168, 169, 180, 181],
    "own": [16, 17, 28, 31, 41, 43, 54, 56, 66, 69, 79, 80, 92, 94, 104, 105, 117, 118, 129, 130, 138, 139, 149, 150, 151, 165, 166, 167, 179, 180, 182, 183],
    "relay": [20, 24, 33, 36, 45, 48, 58, 61, 71, 75, 83, 86, 96, 102, 108, 113, 123, 127, 134, 137, 142, 144, 153, 154, 183, 184, 185, 186, 187, 188, 189, 190],
    "free": [20, 24, 33, 36, 45, 48, 58, 61, 71, 75, 83, 86, 96, 102, 108, 113, 123, 127, 134, 137, 142, 144, 153, 154, 183, 184, 185, 186, 187, 188, 189, 190],
}
EVENTS = tuple(SCHEDULE)


def pick(index, values):
    total = jnp.int32(0)
    for i, v in enumerate(values):
        if v:
            total = total + jnp.where(index == i, jnp.int32(v), jnp.int32(0))
    return total


def kernel(n, x_ref, wg_ref, wu_ref, wd_ref, y_ref, rel_r_ref, rel_l_ref, xv, wv, hv, hold,
           opp_s, dir_s, sum_s, own_s, opp_r, dir_r, sum_r,
           mate_s, mate_r,
           x_sem, px_ss, px_rs, w_sem, out_sem, opp_rs, own_rs, ag_rs, re_ss, re_rs, mate_ss, mate_rs):
    me = lax.axis_index("tp")
    core = lax.rem(lax.axis_index("dp"), 2)
    mate = lax.axis_index("dp") + 1 - 2 * core
    rows, depth_in = x_ref.shape
    hidden, width = wd_ref.shape[0] // 2, wd_ref.shape[1]
    piece = width // n
    nu = rows // UNIT
    kept = nu - TAIL
    gu_steps, dn_steps = hidden // TN, width // TD
    per_piece = dn_steps // n
    steps = gu_steps + dn_steps
    nb = len(BLOCKS)
    total_steps = nb * steps
    last = max(max(v) for v in SCHEDULE.values())
    windows = max(nb, last // steps + 1)
    masks = {e: [sum(1 << (g % steps) for g in v if g // steps == b) for b in range(windows)] for e, v in SCHEDULE.items()}
    starts = {e: [sum(g // steps < b for g in v) for b in range(windows)] for e, v in SCHEDULE.items()}
    mid = {e: [sum(g // steps < b or (g // steps == b and g % steps < gu_steps) for g in v) for b in range(windows)] for e, v in SCHEDULE.items()}
    row0 = [sum(BLOCKS[:b]) for b in range(nb)]

    def at(offset):
        return lax.rem(me + offset, n)

    def remote(src, dst, ssem, rsem, target):
        return pltpu.make_async_remote_copy(src_ref=src, dst_ref=dst, send_sem=ssem, recv_sem=rsem,
                                            device_id={"tp": target}, device_id_type=MESH)

    def cols(owner):
        return pl.ds(pl.multiple_of(owner * piece, piece), piece)

    def unit_rows(s):
        return pl.ds(pl.multiple_of(s * UNIT, UNIT), UNIT)

    def gu_copies(t, slot):
        c = pl.ds(pl.multiple_of(core * hidden + t * TN, TN), TN)
        return (pltpu.make_async_copy(wg_ref.at[:, c], wv.at[slot, :, 0:TN], w_sem.at[slot]),
                pltpu.make_async_copy(wu_ref.at[:, c], wv.at[slot, :, TN:2 * TN], w_sem.at[slot]))

    third = 2 * TN

    def dn_copies(t, slot):
        p, j = t // per_piece, lax.rem(t, per_piece)
        c = at(pick(p, (2, 1, 3, 0))) * piece + j * TD
        r = pl.ds(pl.multiple_of(core * hidden, TN), hidden)
        return [pltpu.make_async_copy(wd_ref.at[r, pl.ds(pl.multiple_of(c + i * third, TN), third)],
                                      wv.at[slot, i * hidden:(i + 1) * hidden, :], w_sem.at[slot])
                for i in range(TD // third)]

    def start_dn(t, slot):
        for c in dn_copies(t, slot):
            c.start()

    def tile_wait(slot, depth):
        tile = wv.at[slot, 0:depth, :]
        pltpu.make_async_copy(tile, tile, w_sem.at[slot]).wait()

    def start_gu(t, slot):
        for c in gu_copies(t, slot):
            c.start()

    def x_copy(b, r):
        return pltpu.make_async_copy(x_ref.at[pl.ds(pl.multiple_of(pick(b, row0), UNIT), r), :], xv.at[pl.ds(0, r), :], x_sem)

    def push_copy(b, r):
        return pltpu.make_async_remote_copy(
            src_ref=x_ref.at[pl.ds(pl.multiple_of(pick(b, row0), UNIT), r), :], dst_ref=xv.at[pl.ds(r, r), :],
            send_sem=px_ss, recv_sem=px_rs, device_id={"dp": mate}, device_id_type=MESH)

    def mate_copy(b, t, r):
        q = lax.rem(b * dn_steps + t, MATE)
        return pltpu.make_async_remote_copy(
            src_ref=mate_s.at[q, pl.ds(0, r), :], dst_ref=mate_r.at[q, pl.ds(0, r), :],
            send_sem=mate_ss.at[q], recv_sem=mate_rs.at[q], device_id={"dp": mate}, device_id_type=MESH)

    def opp_copy(s, slot, par, c):
        return remote(opp_s.at[slot, :, c], opp_r.at[slot, :, c], out_sem.at[slot // 2], opp_rs.at[slot // 2], at(1 + 2 * par))

    def dir_copy(s, slot, par, c):
        return remote(dir_s.at[slot, :, c], dir_r.at[slot, :, c], out_sem.at[slot // 2], own_rs.at[slot // 2], at(3 - 2 * par))

    def sum_copy(s, slot, par):
        return remote(sum_s.at[slot], sum_r.at[slot], out_sem.at[slot // 2], own_rs.at[slot // 2], at(1 + 2 * par))

    def own_copy(s, slot, side):
        return remote(own_s.at[slot], y_ref.at[unit_rows(s), cols(me)], out_sem.at[slot // 2], ag_rs.at[slot // 2], at(1 + 2 * side))

    def keep_copy(s, slot, side):
        rel = (rel_r_ref, rel_l_ref)[side].at[(s - kept) // 2]
        return remote(own_s.at[slot], rel, out_sem.at[slot // 2], ag_rs.at[slot // 2], at(1 + 2 * side))

    def relay_copy(s, par):
        view = y_ref.at[unit_rows(s), cols(at(3 - 2 * par))]
        k = lax.rem(s, DEPTH + LAG) // 2
        return remote(view, view, re_ss.at[k], re_rs.at[k], at(1 + 2 * par))

    def loc_copy(s, slot):
        return pltpu.make_async_copy(own_s.at[slot], y_ref.at[unit_rows(s), cols(me)], out_sem.at[slot // 2])

    whole = pl.ds(0, piece)

    def arrived(sem, k, pieces):
        size = hold.at[0:pieces // 2, 0]
        pltpu.make_async_copy(size, size, sem.at[lax.rem(k, DEPTH // 2)]).wait()

    def duo(k):
        return [(2 * k + par, lax.rem(2 * k + par, DEPTH), par) for par in (0, 1)]

    def pair(k):
        arrived(opp_rs, k, 2)
        for s, slot, par in duo(k):
            sum_s[slot] = (hold[slot, 1 + par] + opp_r[slot].astype(F32)).astype(BF16)
            sum_copy(s, slot, par).start()

    def own(k):
        arrived(own_rs, k, 4)
        for s, slot, par in duo(k):
            own_s[slot] = (hold[slot, 3] + sum_r[slot].astype(F32) + dir_r[slot].astype(F32)).astype(BF16)
            own_copy(s, slot, 1 - par).start()
            loc_copy(s, slot).start()

        @pl.when(2 * k < kept)
        def _():
            for s, slot, par in duo(k):
                own_copy(s, slot, par).start()

        @pl.when(2 * k >= kept)
        def _():
            for s, slot, par in duo(k):
                keep_copy(s, slot, par).start()

    def relay(k):
        arrived(ag_rs, k, 4)

        @pl.when(2 * k < kept)
        def _():
            for s, slot, par in duo(k):
                relay_copy(s, par).start()

    def free(k):
        arrived(out_sem, k, 12)

        @pl.when((2 * k >= LAG) & (2 * k < kept + LAG))
        def _():
            i = lax.rem(2 * k - LAG, DEPTH + LAG) // 2
            for sem in (re_ss, re_rs):
                pltpu.make_async_copy(hold.at[0, 0], hold.at[0, 0], sem.at[i]).wait()

    actions = {"pair": pair, "own": own, "relay": relay, "free": free}

    def events(t, mask, done):
        hits = [lax.shift_right_logical(mask[e], t) & 1 for e in EVENTS]

        @pl.when(sum(hits) > 0)
        def _():
            for e, hit, c in zip(EVENTS, hits, done):
                @pl.when(hit == 1)
                def _(e=e, c=c):
                    actions[e](c)

        return tuple(c + hit for c, hit in zip(done, hits))

    def state(b):
        return {e: pick(b, masks[e]) for e in EVENTS}, b * steps

    def gu_phase(b, r):
        mask, base = state(b)
        x_copy(b, r).wait()

        def hidden_rows(lo, hi, t, slot):
            xb = xv[lo:hi, :]
            gate = jnp.dot(xb, wv[slot, :, 0:TN], preferred_element_type=F32)
            up = jnp.dot(xb, wv[slot, :, TN:2 * TN], preferred_element_type=F32)
            hv[lo:hi, pl.ds(pl.multiple_of(t * TN, TN), TN)] = (jax.nn.silu(gate) * up).astype(BF16)

        @pl.when(b > 0)
        def _():
            push_copy(b, r).wait()

        if r == BLOCKS[0]:
            @pl.when(b == 0)
            def _():
                start_gu(jnp.int32(1), jnp.int32(1))
                tile_wait(jnp.int32(0), depth_in)
                start_gu(jnp.int32(2), jnp.int32(2))
                hidden_rows(0, r, jnp.int32(0), jnp.int32(0))
                push_copy(b, r).wait()
                hidden_rows(r, 2 * r, jnp.int32(0), jnp.int32(0))

        def gu_step(t, done):
            slot = lax.rem(base + t, WBUF)
            tile_wait(slot, depth_in)
            ahead = t + WBUF - 1
            later = lax.rem(base + ahead, WBUF)

            @pl.when(ahead < gu_steps)
            def _():
                start_gu(ahead, later)

            @pl.when(ahead >= gu_steps)
            def _():
                start_dn(ahead - gu_steps, later)

            hidden_rows(0, 2 * r, t, slot)

            @pl.when((t == 0) & (b > 0))
            def _():
                switch(b - 1, lambda b, r: merge(b, dn_steps - 1, r))

            return events(t, mask, done)

        lax.fori_loop(jnp.where(b == 0, 1, 0), gu_steps, gu_step, tuple(pick(b, starts[e]) for e in EVENTS))

    def merge(b, t, r):
        first = pick(b, [v // UNIT for v in row0])
        q = lax.rem(b * dn_steps + t, MATE)
        mate_copy(b, t, r).wait()
        for k in range(r // UNIT):
            s, par = first + k, k % 2
            slot = lax.rem(s, DEPTH)
            both = hold[slot, t] + mate_r[q, k * UNIT:(k + 1) * UNIT, :].astype(F32)
            if t == 0:
                opp_s[slot] = both.astype(BF16)
                opp_copy(s, slot, par, whole).start()
            elif t == 2 - par:
                dir_s[slot] = both.astype(BF16)
                dir_copy(s, slot, par, whole).start()
            else:
                hold[slot, t] = both

    def dn_phase(b, r):
        units = r // UNIT
        first = pick(b, [v // UNIT for v in row0])
        mask, base = state(b)

        def dn_step(t, done):
            g = base + gu_steps + t
            slot = lax.rem(g, WBUF)
            tile_wait(slot, dn_steps // n * hidden * TD // (2 * TN))
            ahead = t + WBUF - 1
            later = lax.rem(g + WBUF - 1, WBUF)

            @pl.when(ahead < dn_steps)
            def _():
                start_dn(ahead, later)

            @pl.when((ahead >= dn_steps) & (b + 1 < nb))
            def _():
                start_gu(ahead - dn_steps, later)

            q = lax.rem(b * dn_steps + t, MATE)
            for i in range(TD // third):
                term = jnp.dot(hv[0:2 * r, :], wv[slot, i * hidden:(i + 1) * hidden, :], preferred_element_type=F32)
                c = slice(i * third, (i + 1) * third)
                for k in range(units):
                    hold[lax.rem(first + k, DEPTH), t, :, c] = term[k * UNIT:(k + 1) * UNIT, :]
                mate_s[q, 0:r, c] = term[r:2 * r, :].astype(BF16)
            mate_copy(b, t, r).start()
            for done_tile in range(dn_steps - 1):
                @pl.when(t == done_tile + 1)
                def _(done_tile=done_tile):
                    merge(b, done_tile, r)
                    if done_tile == 0:
                        for r2 in sorted(set(BLOCKS)):
                            @pl.when(pick(b + 1, [v == r2 for v in BLOCKS]) == 1)
                            def _(r2=r2):
                                x_copy(b + 1, r2).start()
                                push_copy(b + 1, r2).start()
            return events(gu_steps + t, mask, done)

        lax.fori_loop(0, dn_steps, dn_step, tuple(pick(b, mid[e]) for e in EVENTS))

    def switch(b, phase):
        for r in sorted(set(BLOCKS)):
            @pl.when(pick(b, [v == r for v in BLOCKS]) == 1)
            def _(r=r):
                phase(b, r)

    x_copy(jnp.int32(0), BLOCKS[0]).start()
    start_gu(jnp.int32(0), jnp.int32(0))
    barrier = pltpu.get_barrier_semaphore()
    for other in ({"tp": at(1)}, {"tp": at(n - 1)}, {"dp": mate}):
        pl.semaphore_signal(barrier, inc=1, device_id=other, device_id_type=MESH)
    pl.semaphore_wait(barrier, 3)
    push_copy(jnp.int32(0), BLOCKS[0]).start()

    def outer(b, _):
        switch(b, gu_phase)
        switch(b, dn_phase)
        return 0

    lax.fori_loop(0, nb, outer, 0)
    merge(jnp.int32(nb - 1), dn_steps - 1, BLOCKS[-1])

    def tail(g, done):
        b = g // steps
        return events(lax.rem(g, steps), {e: pick(b, masks[e]) for e in EVENTS}, done)

    lax.fori_loop(total_steps, last + 1, tail, tuple(jnp.int32(sum(g < total_steps for g in v)) for v in SCHEDULE.values()))


def copy_kernel(n, y_ref, rel_r_ref, rel_l_ref, out_ref, rows_v, units_v, r_sem, w_sem, ur_sem, uw_sem):
    me = lax.axis_index("tp")
    rows, width = y_ref.shape
    piece = width // n
    full = rows - TAIL * UNIT
    jobs = []
    for i in range(full // CHUNK):
        r = pl.ds(i * CHUNK, CHUNK)
        jobs.append((y_ref.at[r, :], rows_v.at[i], out_ref.at[r, :], r_sem.at[i], w_sem.at[i]))
    for i in range(TAIL):
        r = pl.ds(full + i * UNIT, UNIT)
        for k, offset in enumerate((0, 1, n - 1)):
            c = pl.ds(pl.multiple_of(lax.rem(me + offset, n) * piece, piece), piece)
            src = y_ref.at[r, c]
            if offset == n - 1 and i % 2 == 0:
                src = rel_r_ref.at[i // 2]
            if offset == 1 and i % 2 == 1:
                src = rel_l_ref.at[i // 2]
            jobs.append((src, units_v.at[i, k], out_ref.at[r, c], ur_sem.at[i, k], uw_sem.at[i, k]))
    jobs = jobs[full // CHUNK:] + jobs[:full // CHUNK]
    for src, buf, dst, rs, ws in jobs:
        pltpu.make_async_copy(src, buf, rs).start()
    for src, buf, dst, rs, ws in jobs:
        pltpu.make_async_copy(src, buf, rs).wait()
        pltpu.make_async_copy(buf, dst, ws).start()
    for src, buf, dst, rs, ws in jobs:
        pltpu.make_async_copy(buf, dst, ws).wait()


def finish_kernel(n, from_l_ref, from_r_ref, out_in_ref, out_ref, sem):
    me = lax.axis_index("tp")
    rows, width = out_ref.shape
    piece = width // n
    c = pl.ds(pl.multiple_of(lax.rem(me + 2, n) * piece, piece), piece)
    copies = []
    for i in range(TAIL):
        src = (from_l_ref, from_r_ref)[i % 2].at[i // 2]
        copies.append(pltpu.make_async_copy(src, out_ref.at[pl.ds(rows - (TAIL - i) * UNIT, UNIT), c], sem.at[i]))
    for copy in copies:
        copy.start()
    for copy in copies:
        copy.wait()


def solution(mesh):
    n = mesh.shape["tp"]

    def step(x, w_gate, w_up, w_down):
        rows, din = x.shape
        hidden, width = w_down.shape
        piece = width // n
        rmax = max(BLOCKS)
        ring = pltpu.VMEM((DEPTH, UNIT, piece), BF16)
        dma = pltpu.SemaphoreType.DMA
        rel = jax.ShapeDtypeStruct((TAIL // 2, UNIT, piece), BF16)
        anywhere = pl.BlockSpec(memory_space=pl.ANY)
        y, rel_r, rel_l = pl.pallas_call(
            functools.partial(kernel, n),
            out_shape=(jax.ShapeDtypeStruct((rows, width), BF16), rel, rel),
            in_specs=[anywhere] * 4,
            out_specs=(anywhere,) * 3,
            scratch_shapes=[
                pltpu.VMEM((2 * rmax, din), BF16),
                pltpu.VMEM((WBUF, din, 2 * TN), BF16),
                pltpu.VMEM((2 * rmax, hidden // 2), BF16),
                pltpu.VMEM((DEPTH, n, UNIT, piece), F32),
                ring, ring, ring, ring, ring, ring, ring,
                pltpu.VMEM((MATE, rmax, TD), BF16), pltpu.VMEM((MATE, rmax, TD), BF16),
                dma, dma, dma, dma((WBUF,)), dma((DEPTH // 2,)), dma((DEPTH // 2,)), dma((DEPTH // 2,)), dma((DEPTH // 2,)),
                dma(((DEPTH + LAG) // 2,)), dma(((DEPTH + LAG) // 2,)), dma((MATE + 2,)), dma((MATE + 2,)),
            ],
            compiler_params=pltpu.CompilerParams(
                collective_id=0, has_side_effects=True, vmem_limit_bytes=63 * 2**20),
            cost_estimate=pl.CostEstimate(flops=6 * rows * din * hidden, bytes_accessed=7 * 6 * din * hidden, transcendentals=0),
        )(x, w_gate, w_up, w_down)
        from_l = lax.ppermute(rel_r, "tp", [(i, (i + 1) % n) for i in range(n)])
        from_r = lax.ppermute(rel_l, "tp", [(i, (i - 1) % n) for i in range(n)])
        whole = (rows - TAIL * UNIT) // CHUNK
        out = pl.pallas_call(
            functools.partial(copy_kernel, n),
            out_shape=jax.ShapeDtypeStruct((rows, width), BF16),
            in_specs=[anywhere] * 3,
            out_specs=anywhere,
            scratch_shapes=[
                pltpu.VMEM((whole, CHUNK, width), BF16),
                pltpu.VMEM((TAIL, 3, UNIT, piece), BF16),
                dma((whole,)), dma((whole,)), dma((TAIL, 3)), dma((TAIL, 3)),
            ],
            compiler_params=pltpu.CompilerParams(vmem_limit_bytes=32 * 2**20),
            cost_estimate=pl.CostEstimate(flops=10**10, bytes_accessed=4 * rows * width, transcendentals=0),
        )(y, *(pltpu.with_memory_space_constraint(v, pltpu.HBM) for v in (rel_r, rel_l)))
        vmem = pl.BlockSpec(memory_space=pltpu.VMEM)
        from_l = pltpu.with_memory_space_constraint(from_l, pltpu.VMEM)
        from_r = pltpu.with_memory_space_constraint(from_r, pltpu.VMEM)
        return pl.pallas_call(
            functools.partial(finish_kernel, n),
            out_shape=jax.ShapeDtypeStruct((rows, width), BF16),
            in_specs=[vmem, vmem, anywhere],
            out_specs=anywhere,
            input_output_aliases={2: 0},
            scratch_shapes=[dma((TAIL,))],
        )(from_l, from_r, out)

    return jax.shard_map(
        step,
        mesh=mesh,
        in_specs=(P("dp", None), P(None, "tp"), P(None, "tp"), P("tp", None)),
        out_specs=P("dp", None),
        check_vma=False,
    )
```
